128 devices in a mesh: blk: 32 (over x, z, core), grp: 4 (over y).
Axes of the slice: x: 4, y: 4, z: 4, core: 2. Of those that a mesh axis runs over, the one named last changes fastest.
Arguments:
- statistics: float32 [4, 64, 512, 512], P('grp', 'blk'), as said below
- gradients: bfloat16 [4, 16, 512, 14336], P('grp', None, None, 'blk'), may hold values from -6 to 6
- live_counts: int32 [4, 32], P('grp'), may hold values from 0 to 2, as said below
- slot_row: int32 [4, 64], P('grp'), may hold values from 0 to 15, as said below
- sweeps: int32 [4, 64], P('grp', 'blk'), may hold values from 1 to 2, as said below
Outputs:
- updates: bfloat16 [4, 16, 512, 14336], P('grp', None, None, 'blk')
- off_max: float32 [2], replicated
The draws below stay inside these ranges and needn't reach their ends.
Inputs may be any that keep to these rules, and one draw needn't show every extreme that they name: `live_counts`: the live slots of one index of grp number exactly 16; in every draw some device of each grp index has 2 live slots. `slot_row`: over the live slots of one index of grp each row block 0 to 15 appears exactly once. In each index of grp some live slot has 2 sweeps. `statistics`: every block is symmetric positive definite.
All inputs are finite; a program needn't handle non-finite values.
Results may differ from the reference program's by a relative error of at most 0.0051.
Values may be sent and summed in bfloat16 or wider, within the bound.
A program may use at most 192 MiB of HBM per device.

```python
import jax
import jax.numpy as jnp
from jax import lax

FF = 14336
BLOCK = 512
SLOTS = 2
ROWB = 16
MAXS = 2
N_BLK = 32
N_GRP = 4


def layout(base_key):
    slot_total = N_BLK * SLOTS

    def one_group(row_key):
        keys_list = jax.random.split(row_key, 5)
        heavy_owner = jax.random.randint(keys_list[0], (), 0, N_BLK)
        partner_owner = (heavy_owner + N_BLK // 2) % N_BLK
        priority = jax.random.permutation(keys_list[1], slot_total).astype(jnp.int32)
        slot_ids = lax.iota(jnp.int32, slot_total)
        owner_of = slot_ids // SLOTS
        local_slot = slot_ids % SLOTS
        priority = jnp.where(owner_of == heavy_owner, local_slot - SLOTS, priority)
        priority = jnp.where(owner_of == partner_owner, slot_total + local_slot, priority)
        ranking = jnp.argsort(priority, stable=True)
        picked = jnp.zeros((slot_total,), jnp.int32).at[ranking[:ROWB]].set(1)
        counts = jnp.sum(picked.reshape(N_BLK, SLOTS), axis=1).astype(jnp.int32)
        offsets = jnp.cumsum(counts) - counts
        live_slot = local_slot < counts[owner_of]
        row_order = jax.random.permutation(keys_list[2], ROWB).astype(jnp.int32)
        position = jnp.clip(offsets[owner_of] + local_slot, 0, ROWB - 1)
        filler = jax.random.randint(keys_list[3], (slot_total,), 0, ROWB)
        rows_drawn = jnp.where(live_slot, row_order[position], filler).astype(jnp.int32)
        sweep_drawn = jax.random.randint(keys_list[4], (slot_total,), 1, MAXS + 1)
        sweep_drawn = jnp.where(slot_ids == heavy_owner * SLOTS, MAXS, sweep_drawn).astype(jnp.int32)
        return (counts, rows_drawn, sweep_drawn)
    return jax.vmap(one_group)(jax.random.split(jax.random.fold_in(base_key, 11), N_GRP))


def draw_live_counts(key, part):
    return layout(key)[0]


def draw_slot_row(key, part):
    return layout(key)[1]


def draw_sweeps(key, part):
    return layout(key)[2]


def draw_statistics(key, part):
    slot_total = N_BLK * SLOTS
    samples = 2 * BLOCK
    item_keys = jax.random.split(jax.random.fold_in(key, 5), N_GRP * slot_total)

    def one_block(item_key):
        keys_list = jax.random.split(item_key, 2)
        noise = jax.random.normal(keys_list[0], (BLOCK, samples), jnp.float32)
        scales = jnp.exp(jax.random.uniform(keys_list[1], (BLOCK,), jnp.float32, 0.0, jnp.log(10.0)))
        product = jnp.dot(noise, noise.T, precision=lax.Precision.HIGHEST) / samples
        product = 0.5 * (product + product.T)
        return scales[:, None] * product * scales[None, :] + 0.05 * jnp.eye(BLOCK, dtype=jnp.float32)
    blocks_all = lax.map(one_block, item_keys)
    return blocks_all.reshape(N_GRP, slot_total, BLOCK, BLOCK)


def shard_levels(own_key, shape, shards, least, high):
    gain = 1.0
    for axis_at, shards_of in shards:
        steps = jax.random.uniform(jax.random.fold_in(jax.random.fold_in(own_key, 6), axis_at), (shards_of,), jnp.float32, least / len(shards), high / len(shards))
        gain = gain * jnp.repeat(jnp.exp(steps), shape[axis_at] // shards_of).reshape((-1,) + (1,) * (len(shape) - 1 - axis_at))
    return gain


def scatter_about(key, shape, spread, bound, cuts=(), kind=jnp.bfloat16):
    factor_of = shard_levels(key, shape, cuts, -0.22, 0.18) if cuts else 1.0
    drawn = jax.random.normal(key, shape, jnp.float32) * spread * factor_of
    return jnp.minimum(jnp.maximum(drawn, -bound), bound).astype(kind)


def setup_inputs(seed: int = 0) -> dict:
    arg_keys = jax.random.split(jax.random.key(seed), 6)
    statistics = draw_statistics(jax.random.fold_in(arg_keys[5], 71), 0)
    gradients = scatter_about(arg_keys[1], (N_GRP, ROWB, BLOCK, FF), 1.0, 6.0, ((0, 4), (3, 32)))
    live_counts = draw_live_counts(jax.random.fold_in(arg_keys[5], 71), 0)
    slot_row = draw_slot_row(jax.random.fold_in(arg_keys[5], 71), 0)
    sweeps = draw_sweeps(jax.random.fold_in(arg_keys[5], 71), 0)
    return dict(statistics=statistics, gradients=gradients, live_counts=live_counts, slot_row=slot_row, sweeps=sweeps)


damping = 0.01
pairings = ((0, 1, 2, 3), (0, 2, 1, 3), (0, 3, 1, 2))
highest = lax.Precision.HIGHEST

def regroup_cols(values, pairing, group_width):
    return jnp.concatenate([values[:, member * group_width:(member + 1) * group_width] for member in pairing], axis=1)

def regroup(values, pairing, group_width):
    stacked = jnp.concatenate([values[member * group_width:(member + 1) * group_width] for member in pairing], axis=0)
    return regroup_cols(stacked, pairing, group_width)

def generator(square_sub):
    group_width = square_sub.shape[-1] // 2
    diagonal = jnp.diagonal(square_sub, axis1=1, axis2=2)
    lower_diag = diagonal[:, :group_width, None]
    upper_diag = diagonal[:, None, group_width:]
    coupling = square_sub[:, :group_width, group_width:]
    difference = upper_diag - lower_diag
    bottom = difference * difference + 4.0 * coupling * coupling + damping * (lower_diag + upper_diag) ** 2
    angles = coupling * difference / bottom
    blank = jnp.zeros_like(angles)
    top_half = jnp.concatenate([blank, angles], axis=2)
    low_half = jnp.concatenate([-jnp.swapaxes(angles, 1, 2), blank], axis=2)
    return jnp.concatenate([top_half, low_half], axis=1)

def cayley(skew_part):
    order_size = skew_part.shape[-1]
    identity = jnp.eye(order_size, dtype=jnp.float32)
    square = jnp.einsum('hij,hjk->hik', skew_part, skew_part, precision=highest)
    numerator = identity + skew_part + 0.25 * square
    denominator = identity - 0.25 * square
    factor = jnp.linalg.cholesky(denominator)
    return jax.scipy.linalg.cho_solve((factor, True), numerator)

def rotate_round(matrix, vectors, pairing):
    block_size = matrix.shape[0]
    group_width = block_size // 4
    restore = [pairing.index(member) for member in range(4)]
    matrix = regroup(matrix, pairing, group_width)
    vectors = regroup_cols(vectors, pairing, group_width)
    half_size = 2 * group_width
    square_sub = jnp.stack([matrix[:half_size, :half_size], matrix[half_size:, half_size:]])
    rotation = cayley(generator(square_sub))
    row_part = jnp.einsum('hpq,hpc->hqc', rotation, matrix.reshape(2, half_size, block_size), precision=highest)
    row_part = row_part.reshape(block_size, block_size)
    matrix = jnp.einsum('rhp,hpq->rhq', row_part.reshape(block_size, 2, half_size), rotation, precision=highest)
    matrix = matrix.reshape(block_size, block_size)
    vectors = jnp.einsum('rhp,hpq->rhq', vectors.reshape(block_size, 2, half_size), rotation, precision=highest)
    vectors = vectors.reshape(block_size, block_size)
    return (regroup(matrix, restore, group_width), regroup_cols(vectors, restore, group_width))

def one_sweep(matrix, vectors):
    for pairing in pairings:
        matrix, vectors = rotate_round(matrix, vectors, pairing)
    return (matrix, vectors)

def off_norm(matrix):
    block_size = matrix.shape[0]
    on_diagonal = lax.broadcasted_iota(jnp.int32, (block_size, block_size), 0) == lax.broadcasted_iota(jnp.int32, (block_size, block_size), 1)
    outside = jnp.where(on_diagonal, 0.0, matrix)
    return jnp.sqrt(jnp.sum(outside * outside) / jnp.sum(matrix * matrix))

def root_factor(matrix, vectors):
    scales = jnp.power(jnp.diagonal(matrix), -0.25)
    return jnp.dot(vectors * scales[None, :], vectors.T, precision=highest).astype(jnp.bfloat16)

def pick(group_stats, group_slots):
    return jnp.take(group_stats, group_slots, axis=0)

def reference(statistics, gradients, live_counts, slot_row, sweeps):
    slot_total = N_BLK * SLOTS
    slot_ids = lax.iota(jnp.int32, slot_total)
    row_ids = lax.iota(jnp.int32, ROWB)
    is_live = slot_ids[None, :] % SLOTS < jnp.repeat(live_counts, SLOTS, axis=1)
    matches = (slot_row[:, None, :] == row_ids[None, :, None]) & is_live[:, None, :]
    slot_of = lax.optimization_barrier(jnp.sum(jnp.where(matches, slot_ids[None, None, :], 0), axis=2)).astype(jnp.int32)
    chosen = jax.vmap(pick)(statistics, slot_of)
    chosen_sweeps = jax.vmap(pick)(sweeps, slot_of)
    blocks_flat = chosen.reshape(N_GRP * ROWB, BLOCK, BLOCK)
    sweeps_flat = chosen_sweeps.reshape(N_GRP * ROWB)
    identity = jnp.eye(BLOCK, dtype=jnp.float32)

    def process(payload):
        matrix, sweep_count = payload
        vectors = identity
        off_norms = []
        for sweep_index in range(MAXS):
            new_matrix, new_vectors = one_sweep(matrix, vectors)
            active = sweep_count > sweep_index
            matrix = jnp.where(active, new_matrix, matrix)
            vectors = jnp.where(active, new_vectors, vectors)
            off_norms.append(jnp.where(active, off_norm(new_matrix), jnp.float32(0.0)))
        return (root_factor(matrix, vectors), jnp.stack(off_norms))
    factors, all_norms = lax.map(process, (blocks_flat, sweeps_flat))
    off_max = lax.optimization_barrier(jnp.max(all_norms, axis=0))

    def apply_one(payload):
        factor, gradient = payload
        product = jnp.dot(factor.astype(jnp.float32), gradient.astype(jnp.float32), precision=highest)
        return product.astype(jnp.bfloat16)
    grads_flat = gradients.reshape(N_GRP * ROWB, BLOCK, FF)
    updates = lax.map(apply_one, (factors, grads_flat)).reshape(N_GRP, ROWB, BLOCK, FF)
    return (updates, off_max)
```

```python
import functools
import jax
import jax.numpy as jnp
from jax import lax
from jax.experimental import pallas as pl
from jax.experimental.pallas import tpu as pltpu
from jax.sharding import Mesh
from jax.sharding import PartitionSpec as P

MAXS = 2
GW = 128
damping = 0.01
pairings = ((0, 1, 2, 3), (0, 2, 1, 3), (0, 3, 1, 2))
f32, bf16 = jnp.float32, jnp.bfloat16
TOL = 1e-6
DOUBLINGS = 4


def split(x):
    hi = x.astype(bf16)
    return hi, (x - hi.astype(f32)).astype(bf16)


def dot3(a, b):
    dot = functools.partial(jnp.dot, preferred_element_type=f32)
    return dot(a[0], b[0]) + (dot(a[1], b[0]) + dot(a[0], b[1]))


def grp(member):
    return slice(member * GW, (member + 1) * GW)


def eye_mask(size):
    rows = lax.broadcasted_iota(jnp.int32, (size, size), 0)
    return rows == lax.broadcasted_iota(jnp.int32, (size, size), 1)


def sweep_body(slots, m_ref, v_ref, y_ref, t_ref, p_ref):
    mask = eye_mask(GW)
    identity = mask.astype(f32)
    for pairing in pairings:
        jobs = [(s, pairing[2 * h], pairing[2 * h + 1]) for s in slots for h in range(2)]
        angles, alphas = [], []
        peak = None
        for j, (s, a, b) in enumerate(jobs):
            low = jnp.sum(jnp.where(mask, m_ref[s, grp(a), grp(a)], 0.0), axis=1, keepdims=True)
            up = jnp.sum(jnp.where(mask, m_ref[s, grp(b), grp(b)], 0.0), axis=0, keepdims=True)
            c = m_ref[s, grp(a), grp(b)]
            diff = up - low
            both = up + low
            ang = c * diff / (diff * diff + 4.0 * c * c + damping * (both * both))
            ang_t = ang.T
            sa, sat = split(ang), split(ang_t)
            bb = 0.25 * dot3(sa, sat)
            bound = jnp.max(jnp.sum(jnp.abs(bb), axis=0, keepdims=True), axis=1, keepdims=True)
            alpha = 2.0 / (2.0 + bound)
            cc = (1.0 - alpha) * identity - alpha * bb
            sc = split(cc)
            t = identity + cc
            p = dot3(sc, sc)
            for k in range(1, DOUBLINGS):
                sp = split(p)
                t = t + dot3(split(t), sp)
                if k < DOUBLINGS - 1:
                    p = dot3(sp, sp)
            t_ref[j] = t
            p_ref[j] = p
            angles.append((ang, sa, sat))
            alphas.append(alpha)
            peak = bound if peak is None else jnp.maximum(peak, bound)
        rho = jnp.max(peak / (2.0 + peak))
        for _ in range(DOUBLINGS):
            rho = rho * rho

        def more(r):
            for j in range(len(jobs)):
                sp = split(p_ref[j])
                p = dot3(sp, sp)
                p_ref[j] = p
                t = t_ref[j]
                t_ref[j] = t + dot3(split(t), split(p))
            return r * r

        lax.while_loop(lambda r: r > TOL, more, rho)

        rots = []
        for j in range(len(jobs)):
            ang, sa, sat = angles[j]
            w = alphas[j] * t_ref[j]
            x = dot3(split(w), sa)
            q = identity - 0.5 * dot3(sat, split(x))
            p = 2.0 * w - identity
            xt = x.T
            r = jnp.concatenate(
                [jnp.concatenate([p, x], axis=1), jnp.concatenate([-xt, q], axis=1)], axis=0
            )
            rt = jnp.concatenate(
                [jnp.concatenate([p, -x], axis=1), jnp.concatenate([xt, q], axis=1)], axis=0
            )
            rots.append((split(r), split(rt)))
        for j, (s, a, b) in enumerate(jobs):
            cols = jnp.concatenate([m_ref[s, :, grp(a)], m_ref[s, :, grp(b)]], axis=1)
            y = dot3(split(cols), rots[j][0])
            y_ref[s, :, grp(a)] = y[:, :GW]
            y_ref[s, :, grp(b)] = y[:, GW:]
        for j, (s, a, b) in enumerate(jobs):
            rows = jnp.concatenate([y_ref[s, grp(a), :], y_ref[s, grp(b), :]], axis=0)
            z = dot3(rots[j][1], split(rows))
            m_ref[s, grp(a), :] = z[:GW]
            m_ref[s, grp(b), :] = z[GW:]
        for j, (s, a, b) in enumerate(jobs):
            cols = jnp.concatenate([v_ref[s, :, grp(a)], v_ref[s, :, grp(b)]], axis=1)
            y = dot3(split(cols), rots[j][0])
            v_ref[s, :, grp(a)] = y[:, :GW]
            v_ref[s, :, grp(b)] = y[:, GW:]


def off_norm(matrix, mask):
    square = matrix * matrix
    off = jnp.sum(jnp.where(mask, 0.0, square))
    return jnp.sqrt(off / jnp.sum(square))


def finish(slots, m_ref, v_ref, f_ref, mask):
    for s in slots:
        diagonal = jnp.sum(jnp.where(mask, m_ref[s], 0.0), axis=0, keepdims=True)
        eighth = jnp.sqrt(lax.rsqrt(jnp.sqrt(diagonal)))
        hi, lo = split(v_ref[s] * eighth)
        dot = functools.partial(
            lax.dot_general, dimension_numbers=(((1,), (1,)), ((), ())), preferred_element_type=f32
        )
        f_ref[s] = (dot(hi, hi) + (dot(lo, hi) + dot(hi, lo))).astype(bf16)


def jacobi_kernel(counts_ref, stats_ref, f_ref, off_ref, m_ref, v_ref, y_ref, t_ref, p_ref):
    size = stats_ref.shape[1]
    mask = eye_mask(size)
    n0, n1 = counts_ref[0], counts_ref[1]
    for i in range(MAXS):
        for s in range(2):
            off_ref[i, s] = 0.0
    scratch = (m_ref, v_ref, y_ref, t_ref, p_ref)

    @pl.when(n0 > 0)
    def _():
        m_ref[...] = stats_ref[...]
        for s in range(2):
            v_ref[s] = mask.astype(f32)

    def sweep(i, carry):
        a0, a1 = n0 > i, n1 > i
        slot = jnp.where(a0, 0, 1)

        @pl.when(a0 & a1)
        def _():
            sweep_body((0, 1), *scratch)
            off_ref[i, 0] = off_norm(m_ref[0], eye_mask(size))
            off_ref[i, 1] = off_norm(m_ref[1], eye_mask(size))

        @pl.when(a0 != a1)
        def _():
            sweep_body((slot,), *scratch)
            off_ref[i, slot] = off_norm(m_ref[slot], eye_mask(size))

        return carry

    lax.fori_loop(0, MAXS, sweep, 0)

    @pl.when(n0 > 0)
    def _():
        finish((0,), m_ref, v_ref, f_ref, mask)

    @pl.when(n1 > 0)
    def _():
        finish((1,), m_ref, v_ref, f_ref, mask)


def jacobi(counts, stats):
    slots, size, _ = stats.shape
    vm = pl.BlockSpec(memory_space=pltpu.VMEM)
    sm = pl.BlockSpec(memory_space=pltpu.SMEM)
    return pl.pallas_call(
        jacobi_kernel,
        out_shape=(
            jax.ShapeDtypeStruct((slots, size, size), bf16),
            jax.ShapeDtypeStruct((MAXS, slots), f32),
        ),
        in_specs=[sm, vm],
        out_specs=(vm, sm),
        scratch_shapes=[
            pltpu.VMEM((slots, size, size), f32),
            pltpu.VMEM((slots, size, size), f32),
            pltpu.VMEM((slots, size, size), f32),
            pltpu.VMEM((2 * slots, GW, GW), f32),
            pltpu.VMEM((2 * slots, GW, GW), f32),
        ],
        compiler_params=pltpu.CompilerParams(vmem_limit_bytes=48 << 20),
        name="jacobi",
    )(counts, stats)


BLK = ("blk_0", "blk_1", "blk_2")
BLK_GRP = ("blk_0", "blk_1", "blk_2", "grp")


def per_device(statistics, gradients, live_counts, slot_row, sweeps):
    matrices = statistics[0]
    slot_count, block_size, _ = matrices.shape
    row_count = gradients.shape[1]
    blk_rank = lax.axis_index(BLK)
    own_live = lax.dynamic_index_in_dim(live_counts[0], blk_rank, 0, keepdims=False)
    counts = jnp.where(lax.iota(jnp.int32, slot_count) < own_live, sweeps[0], 0)
    factors, offs = jacobi(counts, matrices)
    off_max = lax.pmax(jnp.max(offs, axis=1), BLK_GRP)
    row_ids = lax.iota(jnp.int32, row_count)
    devices = live_counts.shape[1]
    slot_total = devices * slot_count
    slot_ids = lax.iota(jnp.int32, slot_total)
    is_live = slot_ids % slot_count < jnp.repeat(live_counts[0], slot_count)
    matches = (slot_row[0][None, :] == row_ids[:, None]) & is_live[None, :]
    slot_of = jnp.sum(jnp.where(matches, slot_ids[None, :], 0), axis=1)
    piece = block_size // devices
    spread = lax.all_to_all(
        factors.reshape(slot_count, devices, piece, block_size), BLK, 1, 0, tiled=False
    )
    spread = spread.reshape(slot_total, piece, block_size)
    own = jnp.take(spread, slot_of, axis=0)
    chosen = lax.all_gather(own, BLK, axis=1, tiled=True)
    updates = jnp.einsum("kij,kjc->kic", chosen, gradients[0], preferred_element_type=f32)
    return (updates.astype(bf16)[None], off_max)


def solution(mesh):
    split_mesh = Mesh(
        mesh.devices.reshape(4, 4, 2, mesh.shape["grp"]), ("blk_0", "blk_1", "blk_2", "grp")
    )
    return jax.shard_map(
        per_device,
        mesh=split_mesh,
        in_specs=(
            P("grp", BLK, None, None),
            P("grp", None, None, BLK),
            P("grp", None),
            P("grp", None),
            P("grp", BLK),
        ),
        out_specs=(P("grp", None, None, BLK), P()),
        check_vma=False,
    )
```

```python
import functools
import jax
import jax.numpy as jnp
from jax import lax
from jax.experimental import pallas as pl
from jax.experimental.pallas import tpu as pltpu
from jax.sharding import Mesh
from jax.sharding import PartitionSpec as P

MAXS = 2
GW = 128
damping = 0.01
pairings = ((0, 1, 2, 3), (0, 2, 1, 3), (0, 3, 1, 2))
f32, bf16 = jnp.float32, jnp.bfloat16
TOL = 1e-6
DOUBLINGS = 4
TILES = [(i, j) for i in range(4) for j in range(i, 4)]


def split(x):
    hi = x.astype(bf16)
    return hi, (x - hi.astype(f32)).astype(bf16)


def dot3(a, b):
    dot = functools.partial(jnp.dot, preferred_element_type=f32)
    return dot(a[0], b[0]) + (dot(a[1], b[0]) + dot(a[0], b[1]))


def grp(member):
    return slice(member * GW, (member + 1) * GW)


def eye_mask(size):
    rows = lax.broadcasted_iota(jnp.int32, (size, size), 0)
    return rows == lax.broadcasted_iota(jnp.int32, (size, size), 1)


def sweep_body(slots, m_ref, v_ref, y_ref, t_ref, p_ref):
    mask = eye_mask(GW)
    identity = mask.astype(f32)
    for pairing in pairings:
        jobs = [(s, pairing[2 * h], pairing[2 * h + 1]) for s in slots for h in range(2)]
        angles, alphas = [], []
        peak = None
        for j, (s, a, b) in enumerate(jobs):
            low = jnp.sum(jnp.where(mask, m_ref[s, grp(a), grp(a)], 0.0), axis=1, keepdims=True)
            up = jnp.sum(jnp.where(mask, m_ref[s, grp(b), grp(b)], 0.0), axis=0, keepdims=True)
            c = m_ref[s, grp(a), grp(b)]
            diff = up - low
            both = up + low
            ang = c * diff / (diff * diff + 4.0 * c * c + damping * (both * both))
            ang_t = ang.T
            sa, sat = split(ang), split(ang_t)
            bb = 0.25 * dot3(sa, sat)
            bound = jnp.max(jnp.sum(jnp.abs(bb), axis=0, keepdims=True), axis=1, keepdims=True)
            alpha = 2.0 / (2.0 + bound)
            cc = (1.0 - alpha) * identity - alpha * bb
            sc = split(cc)
            t = identity + cc
            p = dot3(sc, sc)
            for k in range(1, DOUBLINGS):
                sp = split(p)
                t = t + dot3(split(t), sp)
                if k < DOUBLINGS - 1:
                    p = dot3(sp, sp)
            t_ref[j] = t
            p_ref[j] = p
            angles.append((ang, sa, sat))
            alphas.append(alpha)
            peak = bound if peak is None else jnp.maximum(peak, bound)
        rho = jnp.max(peak / (2.0 + peak))
        for _ in range(DOUBLINGS):
            rho = rho * rho

        def more(r):
            for j in range(len(jobs)):
                sp = split(p_ref[j])
                p = dot3(sp, sp)
                p_ref[j] = p
                t = t_ref[j]
                t_ref[j] = t + dot3(split(t), split(p))
            return r * r

        lax.while_loop(lambda r: r > TOL, more, rho)

        rots = []
        for j in range(len(jobs)):
            ang, sa, sat = angles[j]
            w = alphas[j] * t_ref[j]
            x = dot3(split(w), sa)
            q = identity - 0.5 * dot3(sat, split(x))
            p = 2.0 * w - identity
            xt = x.T
            r = jnp.concatenate(
                [jnp.concatenate([p, x], axis=1), jnp.concatenate([-xt, q], axis=1)], axis=0
            )
            rt = jnp.concatenate(
                [jnp.concatenate([p, -x], axis=1), jnp.concatenate([xt, q], axis=1)], axis=0
            )
            rots.append((split(r), split(rt)))
        for j, (s, a, b) in enumerate(jobs):
            cols = jnp.concatenate([m_ref[s, :, grp(a)], m_ref[s, :, grp(b)]], axis=1)
            y = dot3(split(cols), rots[j][0])
            y_ref[s, :, grp(a)] = y[:, :GW]
            y_ref[s, :, grp(b)] = y[:, GW:]
        for j, (s, a, b) in enumerate(jobs):
            rows = jnp.concatenate([y_ref[s, grp(a), :], y_ref[s, grp(b), :]], axis=0)
            z = dot3(rots[j][1], split(rows))
            m_ref[s, grp(a), :] = z[:GW]
            m_ref[s, grp(b), :] = z[GW:]
        for j, (s, a, b) in enumerate(jobs):
            cols = jnp.concatenate([v_ref[s, :, grp(a)], v_ref[s, :, grp(b)]], axis=1)
            y = dot3(split(cols), rots[j][0])
            v_ref[s, :, grp(a)] = y[:, :GW]
            v_ref[s, :, grp(b)] = y[:, GW:]


def off_norm(matrix, mask):
    square = matrix * matrix
    off = jnp.sum(jnp.where(mask, 0.0, square))
    return jnp.sqrt(off / jnp.sum(square))


def finish(slots, m_ref, v_ref, f_ref, mask):
    dot = functools.partial(
        lax.dot_general, dimension_numbers=(((1,), (1,)), ((), ())), preferred_element_type=f32
    )
    for s in slots:
        diagonal = jnp.sum(jnp.where(mask, m_ref[s], 0.0), axis=0, keepdims=True)
        eighth = jnp.sqrt(lax.rsqrt(jnp.sqrt(diagonal)))
        hi, lo = split(v_ref[s] * eighth)
        for i in range(4):
            ah, al, bh, bl = hi[grp(i)], lo[grp(i)], hi[i * GW :], lo[i * GW :]
            line = (dot(ah, bh) + (dot(al, bh) + dot(ah, bl))).astype(bf16)
            for j in range(i, 4):
                t = TILES.index((i, j))
                f_ref[s, grp(t), :] = line[:, grp(j - i)]


def note_off(off_ref, i, value):
    rows = lax.broadcasted_iota(jnp.int32, off_ref.shape, 0)
    off_ref[...] = jnp.where(rows == i, jnp.maximum(off_ref[...], value), off_ref[...])


def jacobi_kernel(
    live_ref, row_ref, sweeps_ref, stats_ref,
    f_ref, off_ref, place_ref, m_ref, v_ref, y_ref, t_ref, p_ref, sem,
):
    size = stats_ref.shape[1]
    devices = live_ref.shape[0]
    mask = eye_mask(size)
    rank = (lax.axis_index("blk_0") * 4 + lax.axis_index("blk_1")) * 2 + lax.axis_index("blk_2")
    own = live_ref[rank]
    n0 = jnp.where(own > 0, sweeps_ref[0], 0)
    n1 = jnp.where(own > 1, sweeps_ref[1], 0)

    def load(s):
        return pltpu.make_async_copy(stats_ref.at[s], m_ref.at[s], sem.at[s])

    for s, n in enumerate((n0, n1)):
        pl.when(n > 0)(lambda s=s: load(s).start())

    for k in range(place_ref.shape[0]):
        place_ref[k] = 0

    def note_place(j, carry):
        @pl.when(lax.rem(j, 2) < live_ref[j // 2])
        def _():
            place_ref[row_ref[j]] = lax.rem(j // 2, 2) * devices + (j // 4) * 2 + lax.rem(j, 2)

        return carry

    lax.fori_loop(0, 2 * devices, note_place, 0)
    off_ref[...] = jnp.zeros_like(off_ref)
    scratch = (m_ref, v_ref, y_ref, t_ref, p_ref)

    for s, n in enumerate((n0, n1)):

        @pl.when(n > 0)
        def _(s=s):
            v_ref[s] = mask.astype(f32)
            load(s).wait()

    def sweep(i, carry):
        a0, a1 = n0 > i, n1 > i
        slot = jnp.where(a0, 0, 1)

        @pl.when(a0 & a1)
        def _():
            sweep_body((0, 1), *scratch)
            for s in range(2):
                note_off(off_ref, i, off_norm(m_ref[s], eye_mask(size)))

        @pl.when(a0 != a1)
        def _():
            sweep_body((slot,), *scratch)
            note_off(off_ref, i, off_norm(m_ref[slot], eye_mask(size)))

        return carry

    lax.fori_loop(0, MAXS, sweep, 0)

    @pl.when(n0 > 0)
    def _():
        finish((0,), m_ref, v_ref, f_ref, mask)

    @pl.when(n1 > 0)
    def _():
        finish((1,), m_ref, v_ref, f_ref, mask)


def jacobi(live, slot_row, sweeps, blocks, stats):
    slots, size, _ = stats.shape
    vm = pl.BlockSpec(memory_space=pltpu.VMEM)
    sm = pl.BlockSpec(memory_space=pltpu.SMEM)
    return pl.pallas_call(
        jacobi_kernel,
        out_shape=(
            jax.ShapeDtypeStruct((slots, len(TILES) * GW, GW), bf16),
            jax.ShapeDtypeStruct((8, GW), f32),
            jax.ShapeDtypeStruct((blocks,), jnp.int32),
        ),
        in_specs=[sm, sm, sm, pl.BlockSpec(memory_space=pl.ANY)],
        out_specs=(vm, vm, sm),
        scratch_shapes=[
            pltpu.VMEM((slots, size, size), f32),
            pltpu.VMEM((slots, size, size), f32),
            pltpu.VMEM((slots, size, size), f32),
            pltpu.VMEM((2 * slots, GW, GW), f32),
            pltpu.VMEM((2 * slots, GW, GW), f32),
            pltpu.SemaphoreType.DMA((2,)),
        ],
        compiler_params=pltpu.CompilerParams(vmem_limit_bytes=48 << 20),
        name="jacobi",
    )(live, slot_row, sweeps, stats)


AXES = ("blk_0", "blk_1", "blk_2", "grp")
CHUNKS = 4
MESH_ID = pl.DeviceIdType.MESH


def gather_kernel(ny, idx_ref, f_ref, off_ref, out_ref, omax_ref,
                  spread, g, offs, ostage,
                  s1, r1, s2, r2, sa, ra, sb, rb, sc, rc, sd, rd, se, re,
                  so, ro, sp, rp, sq, rq, lsem):
    x, z, e, y = [lax.axis_index(a) for a in AXES]
    chip = x * 4 + z
    rows = f_ref.shape[1] // 16

    def ident(c, core, yy):
        return (c // 4, lax.rem(c, 4), core, yy)

    def remote(src, dst, send, recv, dev):
        return pltpu.make_async_remote_copy(
            src_ref=src, dst_ref=dst, send_sem=send, recv_sem=recv,
            device_id=dev, device_id_type=MESH_ID,
        )

    twin = ident(chip, 1 - e, y)

    def peer(d):
        return ident(lax.rem(chip + d, 16), e, y)

    def level(d):
        return ident(chip, e, lax.rem(y + d, ny))

    barrier = pltpu.get_barrier_semaphore()

    def greet(d, carry):
        pl.semaphore_signal(barrier, inc=1, device_id=peer(d), device_id_type=MESH_ID)
        return carry

    lax.fori_loop(1, 16, greet, 0)
    for d in range(1, ny):
        pl.semaphore_signal(barrier, inc=1, device_id=level(d), device_id_type=MESH_ID)
    pl.semaphore_signal(barrier, inc=1, device_id=twin, device_id_type=MESH_ID)
    pl.semaphore_wait(barrier, 15 + (ny - 1) + 1)

    def my_rows(c):
        return f_ref.at[:, pl.ds(pl.multiple_of(c * rows, 16), rows), :]

    def spread_copy(d):
        target = lax.rem(chip + d, 16)
        return remote(my_rows(target), spread.at[e, chip], s1.at[d], r1.at[d], peer(d))

    def pass_copy(d):
        source = lax.rem(chip + 16 - d, 16)
        return remote(spread.at[e, source], spread.at[e, source], s2.at[d], r2.at[d], twin)

    def own_copy():
        return remote(my_rows(chip), spread.at[e, chip], s2.at[0], r2.at[0], twin)

    def off_copy(d):
        return remote(off_ref, offs.at[d], so.at[d], ro.at[d], peer(d))

    def go(copy):
        def step(d, carry):
            copy(d).start()
            return carry
        return step

    lax.fori_loop(1, 16, go(spread_copy), 0)
    lax.fori_loop(1, 16, go(off_copy), 0)
    own_copy().start()
    spread[e, chip] = f_ref[:, pl.ds(pl.multiple_of(chip * rows, 16), rows), :]
    offs[0] = off_ref[...]

    def relay_twin(d, carry):
        source = lax.rem(chip + 16 - d, 16)
        remote(my_rows(chip), spread.at[e, source], s1.at[d], r1.at[d], peer(d)).wait_recv()
        pass_copy(d).start()
        return carry

    lax.fori_loop(1, 16, relay_twin, 0)

    def twin_in(d, carry):
        source = lax.rem(chip + 16 - d, 16)
        remote(
            spread.at[1 - e, source], spread.at[1 - e, source], s2.at[d], r2.at[d], twin
        ).wait_recv()
        return carry

    lax.fori_loop(0, 16, twin_in, 0)

    for q in range(CHUNKS):
        for b in range(2):
            k = 4 * q + 2 * e + b
            j = idx_ref[k]
            g[chip, k] = spread[j // 32, lax.rem(j, 32) // 2, lax.rem(j, 2)]

    pos1 = jnp.where(e == 0, x, z)
    pos2 = jnp.where(e == 0, z, x)

    def at(p1, p2):
        p1, p2 = lax.rem(p1, 4), lax.rem(p2, 4)
        return jnp.where(e == 0, p1 * 4 + p2, p2 * 4 + p1)

    def pair(c, q):
        return g.at[c, pl.ds(4 * q + 2 * e, 2)]

    def single(c, q, b):
        return g.at[c, pl.ds(4 * q + 2 * e + b, 1)]

    def first(q, w):
        dev = ident(at(pos1 + 1 + 2 * w, pos2), e, y)
        return remote(pair(chip, q), pair(chip, q), sa.at[q, w], ra.at[q, w], dev)

    def first_in(q, w):
        c = at(pos1 + 3 - 2 * w, pos2)
        return remote(pair(c, q), pair(c, q), sa.at[q, w], ra.at[q, w], twin)

    def second(q, w):
        c = at(pos1 + 3 - 2 * w, pos2)
        dev = ident(at(pos1 + 1 + 2 * w, pos2), e, y)
        return remote(single(c, q, w), single(c, q, w), sb.at[q, w], rb.at[q, w], dev)

    def second_in(q, w):
        c = at(pos1 + 2, pos2)
        return remote(single(c, q, w), single(c, q, w), sb.at[q, w], rb.at[q, w], twin)

    def third(q, o, w):
        c = at(pos1 + o, pos2)
        dev = ident(at(pos1, pos2 + 1 + 2 * w), e, y)
        return remote(pair(c, q), pair(c, q), sc.at[q, o, w], rc.at[q, o, w], dev)

    def third_in(q, o, w):
        c = at(pos1 + o, pos2 + 3 - 2 * w)
        return remote(pair(c, q), pair(c, q), sc.at[q, o, w], rc.at[q, o, w], twin)

    def fourth(q, o, w):
        c = at(pos1 + o, pos2 + 3 - 2 * w)
        dev = ident(at(pos1, pos2 + 1 + 2 * w), e, y)
        return remote(single(c, q, w), single(c, q, w), sd.at[q, o, w], rd.at[q, o, w], dev)

    def fourth_in(q, o, w):
        c = at(pos1 + o, pos2 + 2)
        return remote(single(c, q, w), single(c, q, w), sd.at[q, o, w], rd.at[q, o, w], twin)

    def across(q, core):
        part = g.at[:, pl.ds(4 * q + 2 * core, 2)]
        return remote(part, part, se.at[q], re.at[q], twin)

    def out_copy(q):
        part = (slice(None), pl.ds(4 * q, 4))
        return pltpu.make_async_copy(g.at[part], out_ref.at[part], lsem.at[q])

    def wave0(q, carry):
        for w in range(2):
            first(q, w).start()
            third(q, 0, w).start()
        return carry

    def wave1(q, carry):
        for w in range(2):
            first_in(q, w).wait_recv()
            second(q, w).start()
        for w in range(2):
            third(q, 1, w).start()
            third(q, 3, w).start()
        for w in range(2):
            third_in(q, 0, w).wait_recv()
            fourth(q, 0, w).start()
        return carry

    def wave2(q, carry):
        for w in range(2):
            second_in(q, w).wait_recv()
        for w in range(2):
            third(q, 2, w).start()
        for o in (1, 3):
            for w in range(2):
                third_in(q, o, w).wait_recv()
                fourth(q, o, w).start()
        return carry

    def wave3(q, carry):
        for w in range(2):
            third_in(q, 2, w).wait_recv()
            fourth(q, 2, w).start()
        return carry

    def wave4(q, carry):
        for o in range(4):
            for w in range(2):
                fourth_in(q, o, w).wait_recv()
        across(q, e).start()
        return carry

    def wave5(q, carry):
        across(q, 1 - e).wait_recv()
        out_copy(q).start()
        return carry

    def off_in(d, carry):
        remote(off_ref, offs.at[d], so.at[d], ro.at[d], peer(d)).wait_recv()
        return carry

    lax.fori_loop(1, 16, off_in, 0)
    top = offs[0]
    for d in range(1, 16):
        top = jnp.maximum(top, offs[d])
    ostage[0] = top

    def level_copy(d):
        return remote(ostage.at[0], ostage.at[d], sp.at[d], rp.at[d], level(d))

    lax.fori_loop(0, CHUNKS, wave0, 0)
    for d in range(1, ny):
        level_copy(d).start()

    lax.fori_loop(0, CHUNKS, wave1, 0)

    for d in range(1, ny):
        level_copy(d).wait_recv()
        top = jnp.maximum(top, ostage[d])
    ostage[ny] = top

    def core_copy():
        return remote(ostage.at[ny], ostage.at[ny + 1], sq, rq, twin)

    lax.fori_loop(0, CHUNKS, wave2, 0)
    core_copy().start()
    lax.fori_loop(0, CHUNKS, wave3, 0)
    core_copy().wait_recv()
    omax_ref[...] = jnp.maximum(top, ostage[ny + 1])
    lax.fori_loop(0, CHUNKS, wave4, 0)
    lax.fori_loop(0, CHUNKS, wave5, 0)

    own_copy().wait_send()

    def drain(d, carry):
        spread_copy(d).wait_send()
        pass_copy(d).wait_send()
        off_copy(d).wait_send()
        return carry

    lax.fori_loop(1, 16, drain, 0)
    for d in range(1, ny):
        level_copy(d).wait_send()
    core_copy().wait_send()

    def drain_chunk(q, carry):
        for w in range(2):
            first(q, w).wait_send()
            second(q, w).wait_send()
            for o in range(4):
                third(q, o, w).wait_send()
                fourth(q, o, w).wait_send()
        across(q, e).wait_send()
        out_copy(q).wait()
        return carry

    lax.fori_loop(0, CHUNKS, drain_chunk, 0)


def gather(idx, packed, offs, ny):
    slots, length, width = packed.shape
    rows = length // 16
    blocks = idx.shape[0]
    vm = pl.BlockSpec(memory_space=pltpu.VMEM)
    dma = pltpu.SemaphoreType.DMA
    n = CHUNKS
    return pl.pallas_call(
        functools.partial(gather_kernel, ny),
        out_shape=(
            jax.ShapeDtypeStruct((16, blocks, rows, width), bf16),
            jax.ShapeDtypeStruct(offs.shape, f32),
        ),
        in_specs=[pl.BlockSpec(memory_space=pltpu.SMEM), vm, vm],
        out_specs=(pl.BlockSpec(memory_space=pl.ANY), vm),
        scratch_shapes=[
            pltpu.VMEM((2, 16, slots, rows, width), bf16),
            pltpu.VMEM((16, blocks, rows, width), bf16),
            pltpu.VMEM((16,) + offs.shape, f32),
            pltpu.VMEM((ny + 2,) + offs.shape, f32),
            dma((16,)), dma((16,)), dma((16,)), dma((16,)),
            dma((n, 2)), dma((n, 2)), dma((n, 2)), dma((n, 2)),
            dma((n, 4, 2)), dma((n, 4, 2)), dma((n, 4, 2)), dma((n, 4, 2)),
            dma((n,)), dma((n,)),
            dma((16,)), dma((16,)), dma((ny,)), dma((ny,)), dma, dma,
            dma((n,)),
        ],
        compiler_params=pltpu.CompilerParams(
            collective_id=0, has_side_effects=True, vmem_limit_bytes=32 << 20
        ),
        name="gather_factors",
    )(idx, packed, offs)


def apply_kernel(p_ref, g_ref, u_ref):
    count, _, rows, width = p_ref.shape
    packed = p_ref[...].reshape(count * rows, width)
    tiles = {ij: packed[t * GW : (t + 1) * GW] for t, ij in enumerate(TILES)}
    lines = [
        jnp.concatenate([tiles[i, j] if j >= i else tiles[j, i].T for j in range(4)], axis=1)
        for i in range(4)
    ]
    u_ref[0] = jnp.dot(
        g_ref[0], jnp.concatenate(lines, axis=0), preferred_element_type=f32
    ).astype(bf16)


def apply(packed, gradients):
    blocks, cols, size = gradients.shape
    chips, _, rows, width = packed.shape
    return pl.pallas_call(
        apply_kernel,
        grid=(blocks,),
        out_shape=jax.ShapeDtypeStruct((blocks, cols, size), bf16),
        in_specs=[
            pl.BlockSpec((chips, 1, rows, width), lambda k: (0, k, 0, 0)),
            pl.BlockSpec((1, cols, size), lambda k: (k, 0, 0)),
        ],
        out_specs=pl.BlockSpec((1, cols, size), lambda k: (k, 0, 0)),
        compiler_params=pltpu.CompilerParams(vmem_limit_bytes=32 << 20),
        name="apply_factors",
    )(packed, gradients)


BLK = AXES[:3]


def per_device(ny, statistics, gradients, live_counts, slot_row, sweeps):
    matrices = statistics[0]
    packed, offs, where_of = jacobi(
        live_counts[0], slot_row[0], sweeps[0], gradients.shape[1], matrices
    )
    pieces, tops = gather(where_of, packed, offs, ny)
    updates = apply(pieces, jnp.swapaxes(gradients[0], 1, 2))
    return jnp.swapaxes(updates, 1, 2)[None], tops[:MAXS, 0]


def solution(mesh):
    ny = mesh.shape["grp"]
    split_mesh = Mesh(mesh.devices.reshape(4, 4, 2, ny), AXES)
    return jax.shard_map(
        functools.partial(per_device, ny),
        mesh=split_mesh,
        in_specs=(
            P("grp", BLK, None, None),
            P("grp", None, None, BLK),
            P("grp", None),
            P("grp", None),
            P("grp", BLK),
        ),
        out_specs=(P("grp", None, None, BLK), P()),
        check_vma=False,
    )
```

```python
import functools
import jax
import jax.numpy as jnp
from jax import lax
from jax.experimental import pallas as pl
from jax.experimental.pallas import tpu as pltpu
from jax.sharding import Mesh
from jax.sharding import PartitionSpec as P

MAXS = 2
GW = 128
damping = 0.01
pairings = ((0, 1, 2, 3), (0, 2, 1, 3), (0, 3, 1, 2))
f32, bf16 = jnp.float32, jnp.bfloat16
TOL = 1e-6
EASY = 1.5
TILES = [(i, j) for i in range(4) for j in range(i, 4)]


def split(x):
    hi = x.astype(bf16)
    return hi, (x - hi.astype(f32)).astype(bf16)


def dot(a, b):
    return jnp.dot(a, b, preferred_element_type=f32)


def dot3(a, b):
    return dot(a[0], b[0]) + (dot(a[1], b[0]) + dot(a[0], b[1]))


def dot3_packed(a, b):
    left = jnp.concatenate([a[0], a[1]], axis=1)
    top = jnp.concatenate([b[0], b[1]], axis=1)
    low = jnp.concatenate([b[0], jnp.zeros_like(b[1])], axis=1)
    both = dot(left, jnp.concatenate([top, low], axis=0))
    return both[:, :GW] + both[:, GW:]


def two(a, b):
    return jnp.concatenate([a, b], axis=1)


def apart(pair):
    blank = jnp.zeros((GW, GW), pair.dtype)
    return jnp.concatenate([two(pair[:, :GW], blank), two(blank, pair[:, GW:])], axis=0)


def grp(member):
    return slice(member * GW, (member + 1) * GW)


def eye_mask(size):
    rows = lax.broadcasted_iota(jnp.int32, (size, size), 0)
    return rows == lax.broadcasted_iota(jnp.int32, (size, size), 1)


def inverse_rare(jobs, w_ref, b_ref, p_ref, peak):
    identity = eye_mask(GW).astype(f32)
    alpha = 2.0 / (2.0 + peak)
    for j in jobs:
        c = (1.0 - alpha) * identity - alpha * b_ref[j]
        p_ref[j] = c
        w_ref[j] = identity + c

    def more(r):
        for j in jobs:
            sp = split(p_ref[j])
            p = dot3(sp, sp)
            p_ref[j] = p
            t = w_ref[j]
            w_ref[j] = t + dot3(split(t), split(p))
        return r * r

    rho = peak / (2.0 + peak)
    lax.while_loop(lambda r: r > TOL, more, rho * rho)
    for j in jobs:
        w_ref[j] = alpha * w_ref[j]


def sweep_body(slots, m_ref, v_ref, y_ref, w_ref, b_ref, p_ref, r_ref):
    mask = eye_mask(GW)
    identity = mask.astype(f32)
    eye2 = two(identity, identity)

    def rot(s, h):
        return (
            (r_ref[s, h, 0], r_ref[s, h, 1]),
            (r_ref[s, h, 2], r_ref[s, h, 3]),
        )

    def block(s, rows, cols):
        lines = [two(m_ref[s, grp(a), grp(cols[0])], m_ref[s, grp(a), grp(cols[1])]) for a in rows]
        return jnp.concatenate(lines, axis=0)

    def store(s, rows, cols, value):
        for i, a in enumerate(rows):
            for j, b in enumerate(cols):
                m_ref[s, grp(a), grp(b)] = value[grp(i), grp(j)]

    def settle(s, halves):
        for h in range(2):
            r, rt = rot(s, h)
            store(s, halves[h], halves[h], dot3(rt, split(y_ref[s, h])))
            cols = two(v_ref[s, :, grp(halves[h][0])], v_ref[s, :, grp(halves[h][1])])
            turned = dot3(split(cols), r)
            for i in range(2):
                v_ref[s, :, grp(halves[h][i])] = turned[:, grp(i)]

    last, diagonals = None, {}
    for pairing in pairings:
        halves = (pairing[:2], pairing[2:])
        peak = None
        kept = {}
        for n, s in enumerate(slots):
            ang, mats = [], []
            for h, (a, b) in enumerate(halves):
                if last is None:
                    low = jnp.sum(jnp.where(mask, m_ref[s, grp(a), grp(a)], 0.0), axis=1, keepdims=True)
                    up = jnp.sum(jnp.where(mask, m_ref[s, grp(b), grp(b)], 0.0), axis=0, keepdims=True)
                else:
                    low = jnp.sum(jnp.where(mask, diagonals[n, a], 0.0), axis=1, keepdims=True)
                    up = diagonals[n, b]
                c = m_ref[s, grp(a), grp(b)]
                diff = up - low
                both = up + low
                one = c * diff / (diff * diff + 4.0 * c * c + damping * (both * both))
                sa, sat = split(one), split(one.T)
                bb = 0.25 * dot3_packed(sa, sat)
                b_ref[2 * n + h] = bb
                ang.append((sa, sat))
                mats.append(bb)
            bb = two(*mats)
            bound = jnp.max(jnp.sum(jnp.abs(bb), axis=0, keepdims=True), axis=1, keepdims=True)
            alpha = 2.0 / (2.0 + bound)
            c = (1.0 - alpha) * eye2 - alpha * bb
            cb = c.astype(bf16)
            p = dot(cb, apart(cb))
            t = eye2 + c
            pb = p.astype(bf16)
            stacked = dot(jnp.concatenate([t.astype(bf16), pb], axis=0), apart(pb))
            t = t + stacked[:GW]
            w = alpha * (t + dot(t.astype(bf16), apart(stacked[GW:].astype(bf16))))
            done = two(*[
                dot3_packed(split(mats[h]), split(w[:, grp(h)])) for h in range(2)
            ])
            error = eye2 - w - done
            w = w + dot(w.astype(bf16), apart(error.astype(bf16)))
            for h in range(2):
                w_ref[2 * n + h] = w[:, grp(h)]
            kept[n] = ang
            peak = bound if peak is None else jnp.maximum(peak, bound)
            if last is not None:
                settle(s, last)
        peak = jnp.max(peak)

        @pl.when(peak > EASY)
        def _():
            inverse_rare(range(2 * len(slots)), w_ref, b_ref, p_ref, peak)

        for n, s in enumerate(slots):
            for h, (sa, sat) in enumerate(kept[n]):
                w = w_ref[2 * n + h]
                x = dot3_packed(split(w), sa)
                sx = split(x)
                q = identity - 0.5 * dot3_packed(sat, sx)
                p = 2.0 * w - identity
                sp, sq, sxt = split(p), split(q), split(x.T)
                for i in range(2):
                    r_ref[s, h, i] = jnp.concatenate([two(sp[i], sx[i]), two(-sxt[i], sq[i])], axis=0)
                    r_ref[s, h, 2 + i] = jnp.concatenate(
                        [two(sp[i], -sx[i]), two(sxt[i], sq[i])], axis=0
                    )
        for n, s in enumerate(slots):
            r0, rt0 = rot(s, 0)
            r1, _ = rot(s, 1)
            z = dot3(rt0, split(dot3(split(block(s, halves[0], halves[1])), r1)))
            for h, r in enumerate((r0, r1)):
                y = dot3(split(block(s, halves[h], halves[h])), r)
                y_ref[s, h] = y
                full = r[0].astype(f32) + r[1].astype(f32)
                row = jnp.sum(full * y, axis=0, keepdims=True)
                for i in range(2):
                    diagonals[n, halves[h][i]] = row[:, grp(i)]
            store(s, halves[0], halves[1], z)
            store(s, halves[1], halves[0], z.T)
        last = halves
    for s in slots:
        settle(s, last)


def off_norm(matrix, mask):
    square = matrix * matrix
    off = jnp.sum(jnp.where(mask, 0.0, square))
    return jnp.sqrt(off / jnp.sum(square))


def finish(slots, m_ref, v_ref, f_ref, mask):
    dot = functools.partial(
        lax.dot_general, dimension_numbers=(((1,), (1,)), ((), ())), preferred_element_type=f32
    )
    for s in slots:
        diagonal = jnp.sum(jnp.where(mask, m_ref[s], 0.0), axis=0, keepdims=True)
        eighth = jnp.sqrt(lax.rsqrt(jnp.sqrt(diagonal)))
        hi, lo = split(v_ref[s] * eighth)
        for i in range(4):
            ah, al, bh, bl = hi[grp(i)], lo[grp(i)], hi[i * GW :], lo[i * GW :]
            line = (dot(ah, bh) + (dot(al, bh) + dot(ah, bl))).astype(bf16)
            for j in range(i, 4):
                t = TILES.index((i, j))
                f_ref[s, grp(t), :] = line[:, grp(j - i)]


def note_off(off_ref, i, value):
    rows = lax.broadcasted_iota(jnp.int32, off_ref.shape, 0)
    off_ref[...] = jnp.where(rows == i, jnp.maximum(off_ref[...], value), off_ref[...])


def jacobi_kernel(
    live_any, row_any, sweeps_any, stats_ref,
    f_ref, off_ref, place_ref, m_ref, v_ref, y_ref, w_ref, b_ref, p_ref, r_ref, live_s, row_s, sweeps_s, sem,
):
    small = [
        pltpu.make_async_copy(src, dst, sem.at[2 + i])
        for i, (src, dst) in enumerate(
            ((live_any, live_s), (row_any, row_s), (sweeps_any, sweeps_s))
        )
    ]
    for copy in small:
        copy.start()
    for copy in small:
        copy.wait()
    live_ref, row_ref, sweeps_ref = live_s.at[0], row_s.at[0], sweeps_s.at[0]
    size = stats_ref.shape[1]
    devices = live_ref.shape[0]
    mask = eye_mask(size)
    rank = (lax.axis_index("blk_0") * 4 + lax.axis_index("blk_1")) * 2 + lax.axis_index("blk_2")
    own = live_ref[rank]
    n0 = jnp.where(own > 0, sweeps_ref[0], 0)
    n1 = jnp.where(own > 1, sweeps_ref[1], 0)

    def load(s):
        return pltpu.make_async_copy(stats_ref.at[s], m_ref.at[s], sem.at[s])

    for s, n in enumerate((n0, n1)):
        pl.when(n > 0)(lambda s=s: load(s).start())

    for k in range(place_ref.shape[0]):
        place_ref[k] = 0

    def note_place(j, carry):
        @pl.when(lax.rem(j, 2) < live_ref[j // 2])
        def _():
            place_ref[row_ref[j]] = lax.rem(j // 2, 2) * devices + (j // 4) * 2 + lax.rem(j, 2)

        return carry

    lax.fori_loop(0, 2 * devices, note_place, 0)
    off_ref[...] = jnp.zeros_like(off_ref)
    scratch = (m_ref, v_ref, y_ref, w_ref, b_ref, p_ref, r_ref)

    for s, n in enumerate((n0, n1)):

        @pl.when(n > 0)
        def _(s=s):
            v_ref[s] = mask.astype(f32)
            load(s).wait()

    def sweep(i, carry):
        a0, a1 = n0 > i, n1 > i
        slot = jnp.where(a0, 0, 1)

        @pl.when(a0 & a1)
        def _():
            sweep_body((0, 1), *scratch)
            for s in range(2):
                note_off(off_ref, i, off_norm(m_ref[s], eye_mask(size)))

        @pl.when(a0 != a1)
        def _():
            sweep_body((slot,), *scratch)
            note_off(off_ref, i, off_norm(m_ref[slot], eye_mask(size)))

        return carry

    lax.fori_loop(0, MAXS, sweep, 0)

    @pl.when(n0 > 0)
    def _():
        finish((0,), m_ref, v_ref, f_ref, mask)

    @pl.when(n1 > 0)
    def _():
        finish((1,), m_ref, v_ref, f_ref, mask)


def jacobi(live, slot_row, sweeps, blocks, stats):
    slots, size, _ = stats.shape
    vm = pl.BlockSpec(memory_space=pltpu.VMEM)
    sm = pl.BlockSpec(memory_space=pltpu.SMEM)
    return pl.pallas_call(
        jacobi_kernel,
        out_shape=(
            jax.ShapeDtypeStruct((slots, len(TILES) * GW, GW), bf16),
            jax.ShapeDtypeStruct((8, GW), f32),
            jax.ShapeDtypeStruct((blocks,), jnp.int32),
        ),
        in_specs=[pl.BlockSpec(memory_space=pltpu.HBM)] * 4,
        out_specs=(vm, vm, sm),
        scratch_shapes=[
            pltpu.VMEM((slots, size, size), f32),
            pltpu.VMEM((slots, size, size), f32),
            pltpu.VMEM((slots, 2, 2 * GW, 2 * GW), f32),
            pltpu.VMEM((2 * slots, GW, GW), f32),
            pltpu.VMEM((2 * slots, GW, GW), f32),
            pltpu.VMEM((2 * slots, GW, GW), f32),
            pltpu.VMEM((slots, 2, 4, 2 * GW, 2 * GW), bf16),
            pltpu.SMEM(live.shape, jnp.int32),
            pltpu.SMEM(slot_row.shape, jnp.int32),
            pltpu.SMEM(sweeps.shape, jnp.int32),
            pltpu.SemaphoreType.DMA((5,)),
        ],
        cost_estimate=pl.CostEstimate(flops=20 * 10**9, bytes_accessed=1 << 20, transcendentals=0),
        compiler_params=pltpu.CompilerParams(vmem_limit_bytes=24 << 20),
        name="jacobi",
    )(live, slot_row, sweeps, stats)


AXES = ("blk_0", "blk_1", "blk_2", "grp")
CHUNKS = 4
WIDE = 8 // CHUNKS
MESH_ID = pl.DeviceIdType.MESH


def gather_kernel(ny, idx_ref, f_ref, off_ref, g, omax_ref,
                  spread, offs, ostage,
                  s1, r1, s2, r2, sa, ra, sb, rb, sc, rc, sd, rd, se, re,
                  so, ro, sp, rp, sq, rq):
    x, z, e, y = [lax.axis_index(a) for a in AXES]
    chip = x * 4 + z
    rows = f_ref.shape[1] // 16

    def ident(c, core, yy):
        return (c // 4, lax.rem(c, 4), core, yy)

    def remote(src, dst, send, recv, dev):
        return pltpu.make_async_remote_copy(
            src_ref=src, dst_ref=dst, send_sem=send, recv_sem=recv,
            device_id=dev, device_id_type=MESH_ID,
        )

    twin = ident(chip, 1 - e, y)

    def peer(d):
        return ident(lax.rem(chip + d, 16), e, y)

    def level(d):
        return ident(chip, e, lax.rem(y + d, ny))

    barrier = pltpu.get_barrier_semaphore()

    def greet(d, carry):
        pl.semaphore_signal(barrier, inc=1, device_id=peer(d), device_id_type=MESH_ID)
        return carry

    lax.fori_loop(1, 16, greet, 0)
    for d in range(1, ny):
        pl.semaphore_signal(barrier, inc=1, device_id=level(d), device_id_type=MESH_ID)
    pl.semaphore_signal(barrier, inc=1, device_id=twin, device_id_type=MESH_ID)
    pl.semaphore_wait(barrier, 15 + (ny - 1) + 1)

    def my_rows(c):
        return f_ref.at[:, pl.ds(pl.multiple_of(c * rows, 16), rows), :]

    def spread_copy(d):
        target = lax.rem(chip + d, 16)
        return remote(my_rows(target), spread.at[e, chip], s1.at[d], r1.at[d], peer(d))

    def pass_copy(d):
        source = lax.rem(chip + 16 - d, 16)
        return remote(spread.at[e, source], spread.at[e, source], s2.at[d], r2.at[d], twin)

    def own_copy():
        return remote(my_rows(chip), spread.at[e, chip], s2.at[0], r2.at[0], twin)

    def off_copy(d):
        return remote(off_ref, offs.at[d], so.at[d], ro.at[d], peer(d))

    def go(copy):
        def step(d, carry):
            copy(d).start()
            return carry
        return step

    lax.fori_loop(1, 16, go(spread_copy), 0)
    lax.fori_loop(1, 16, go(off_copy), 0)
    own_copy().start()
    spread[e, chip] = f_ref[:, pl.ds(pl.multiple_of(chip * rows, 16), rows), :]
    offs[0] = off_ref[...]

    def relay_twin(d, carry):
        source = lax.rem(chip + 16 - d, 16)
        remote(my_rows(chip), spread.at[e, source], s1.at[d], r1.at[d], peer(d)).wait_recv()
        pass_copy(d).start()
        return carry

    lax.fori_loop(1, 16, relay_twin, 0)

    def twin_in(d, carry):
        source = lax.rem(chip + 16 - d, 16)
        remote(
            spread.at[1 - e, source], spread.at[1 - e, source], s2.at[d], r2.at[d], twin
        ).wait_recv()
        return carry

    lax.fori_loop(0, 16, twin_in, 0)

    for q in range(CHUNKS):
        for b in range(WIDE):
            k = WIDE * (2 * q + e) + b
            j = idx_ref[k]
            g[chip, k] = spread[j // 32, lax.rem(j, 32) // 2, lax.rem(j, 2)]

    pos1 = jnp.where(e == 0, x, z)
    pos2 = jnp.where(e == 0, z, x)

    def at(p1, p2):
        p1, p2 = lax.rem(p1, 4), lax.rem(p2, 4)
        return jnp.where(e == 0, p1 * 4 + p2, p2 * 4 + p1)

    def pair(c, q):
        return g.at[c, pl.ds(WIDE * (2 * q + e), WIDE)]

    def single(c, q, b):
        return g.at[c, pl.ds(WIDE * (2 * q + e) + WIDE // 2 * b, WIDE // 2)]

    def first(q, w):
        dev = ident(at(pos1 + 1 + 2 * w, pos2), e, y)
        return remote(pair(chip, q), pair(chip, q), sa.at[q, w], ra.at[q, w], dev)

    def first_in(q, w):
        c = at(pos1 + 3 - 2 * w, pos2)
        return remote(pair(c, q), pair(c, q), sa.at[q, w], ra.at[q, w], twin)

    def second(q, w):
        c = at(pos1 + 3 - 2 * w, pos2)
        dev = ident(at(pos1 + 1 + 2 * w, pos2), e, y)
        return remote(single(c, q, w), single(c, q, w), sb.at[q, w], rb.at[q, w], dev)

    def second_in(q, w):
        c = at(pos1 + 2, pos2)
        return remote(single(c, q, w), single(c, q, w), sb.at[q, w], rb.at[q, w], twin)

    def third(q, o, w):
        c = at(pos1 + o, pos2)
        dev = ident(at(pos1, pos2 + 1 + 2 * w), e, y)
        return remote(pair(c, q), pair(c, q), sc.at[q, o, w], rc.at[q, o, w], dev)

    def third_in(q, o, w):
        c = at(pos1 + o, pos2 + 3 - 2 * w)
        return remote(pair(c, q), pair(c, q), sc.at[q, o, w], rc.at[q, o, w], twin)

    def fourth(q, o, w):
        c = at(pos1 + o, pos2 + 3 - 2 * w)
        dev = ident(at(pos1, pos2 + 1 + 2 * w), e, y)
        return remote(single(c, q, w), single(c, q, w), sd.at[q, o, w], rd.at[q, o, w], dev)

    def fourth_in(q, o, w):
        c = at(pos1 + o, pos2 + 2)
        return remote(single(c, q, w), single(c, q, w), sd.at[q, o, w], rd.at[q, o, w], twin)

    def across(q, core):
        part = g.at[:, pl.ds(WIDE * (2 * q + core), WIDE)]
        return remote(part, part, se.at[q], re.at[q], twin)

    def wave0(q, carry):
        for w in range(2):
            first(q, w).start()
            third(q, 0, w).start()
        return carry

    def wave1(q, carry):
        for w in range(2):
            first_in(q, w).wait_recv()
            second(q, w).start()
        for w in range(2):
            third(q, 1, w).start()
            third(q, 3, w).start()
        for w in range(2):
            third_in(q, 0, w).wait_recv()
            fourth(q, 0, w).start()
        return carry

    def wave2(q, carry):
        for w in range(2):
            second_in(q, w).wait_recv()
        for w in range(2):
            third(q, 2, w).start()
        for o in (1, 3):
            for w in range(2):
                third_in(q, o, w).wait_recv()
                fourth(q, o, w).start()
        return carry

    def wave3(q, carry):
        for w in range(2):
            third_in(q, 2, w).wait_recv()
            fourth(q, 2, w).start()
        return carry

    def wave4(q, carry):
        for o in range(4):
            for w in range(2):
                fourth_in(q, o, w).wait_recv()
        across(q, e).start()
        return carry

    def wave5(q, carry):
        across(q, 1 - e).wait_recv()
        return carry

    def off_in(d, carry):
        remote(off_ref, offs.at[d], so.at[d], ro.at[d], peer(d)).wait_recv()
        return carry

    lax.fori_loop(1, 16, off_in, 0)
    top = offs[0]
    for d in range(1, 16):
        top = jnp.maximum(top, offs[d])
    ostage[0] = top

    def level_copy(d):
        return remote(ostage.at[0], ostage.at[d], sp.at[d], rp.at[d], level(d))

    lax.fori_loop(0, CHUNKS, wave0, 0)
    for d in range(1, ny):
        level_copy(d).start()

    lax.fori_loop(0, CHUNKS, wave1, 0)

    for d in range(1, ny):
        level_copy(d).wait_recv()
        top = jnp.maximum(top, ostage[d])
    ostage[ny] = top

    def core_copy():
        return remote(ostage.at[ny], ostage.at[ny + 1], sq, rq, twin)

    lax.fori_loop(0, CHUNKS, wave2, 0)
    core_copy().start()
    lax.fori_loop(0, CHUNKS, wave3, 0)
    core_copy().wait_recv()
    omax_ref[...] = jnp.maximum(top, ostage[ny + 1])
    lax.fori_loop(0, CHUNKS, wave4, 0)
    lax.fori_loop(0, CHUNKS, wave5, 0)

    own_copy().wait_send()

    def drain(d, carry):
        spread_copy(d).wait_send()
        pass_copy(d).wait_send()
        off_copy(d).wait_send()
        return carry

    lax.fori_loop(1, 16, drain, 0)
    for d in range(1, ny):
        level_copy(d).wait_send()
    core_copy().wait_send()

    def drain_chunk(q, carry):
        for w in range(2):
            first(q, w).wait_send()
            second(q, w).wait_send()
            for o in range(4):
                third(q, o, w).wait_send()
                fourth(q, o, w).wait_send()
        across(q, e).wait_send()
        return carry

    lax.fori_loop(0, CHUNKS, drain_chunk, 0)


def gather(idx, packed, offs, ny):
    slots, length, width = packed.shape
    rows = length // 16
    blocks = idx.shape[0]
    vm = pl.BlockSpec(memory_space=pltpu.VMEM)
    dma = pltpu.SemaphoreType.DMA
    n = CHUNKS
    return pl.pallas_call(
        functools.partial(gather_kernel, ny),
        out_shape=(
            jax.ShapeDtypeStruct((16, blocks, rows, width), bf16),
            jax.ShapeDtypeStruct(offs.shape, f32),
        ),
        in_specs=[pl.BlockSpec(memory_space=pltpu.SMEM), vm, vm],
        out_specs=(vm, vm),
        scratch_shapes=[
            pltpu.VMEM((2, 16, slots, rows, width), bf16),
            pltpu.VMEM((16,) + offs.shape, f32),
            pltpu.VMEM((ny + 2,) + offs.shape, f32),
            dma((16,)), dma((16,)), dma((16,)), dma((16,)),
            dma((n, 2)), dma((n, 2)), dma((n, 2)), dma((n, 2)),
            dma((n, 4, 2)), dma((n, 4, 2)), dma((n, 4, 2)), dma((n, 4, 2)),
            dma((n,)), dma((n,)),
            dma((16,)), dma((16,)), dma((ny,)), dma((ny,)), dma, dma,
        ],
        compiler_params=pltpu.CompilerParams(
            collective_id=0, has_side_effects=True, vmem_limit_bytes=16 << 20
        ),
        cost_estimate=pl.CostEstimate(flops=20 * 10**9, bytes_accessed=1 << 20, transcendentals=0),
        name="gather_factors",
    )(idx, packed, offs)


def apply_kernel(p_ref, o_ref, g_ref, u_any, tops_ref, u_ref, f_ref, out_sem):
    blocks = g_ref.shape[0]
    rows = p_ref.shape[2]

    def save(k):
        return pltpu.make_async_copy(u_ref.at[k], u_any.at[k], out_sem.at[k])

    for i in range(MAXS):
        tops_ref[i] = jnp.max(o_ref[i : i + 1, :])

    def assemble(k, slot):
        packed = p_ref[:, k].reshape(p_ref.shape[0] * rows, GW)
        for t, (i, j) in enumerate(TILES):
            tile = packed[grp(t)]
            f_ref[slot, grp(i), grp(j)] = tile
            if i != j:
                f_ref[slot, grp(j), grp(i)] = tile.T

    def turn(k, slot):
        u_ref[k] = dot(g_ref[k], f_ref[slot]).astype(bf16)

    assemble(0, 0)

    def step(n, carry):
        k = 2 * n
        assemble(k + 1, 1)
        turn(k, 0)
        assemble(jnp.minimum(k + 2, blocks - 1), 0)
        turn(k + 1, 1)
        save(k).start()
        save(k + 1).start()
        return carry

    lax.fori_loop(0, blocks // 2, step, 0)
    for k in range(blocks):
        save(k).wait()


def apply(packed, tops, gradients):
    blocks, cols, size = gradients.shape
    anywhere = pl.BlockSpec(memory_space=pl.ANY)
    vm = pl.BlockSpec(memory_space=pltpu.VMEM)
    return pl.pallas_call(
        apply_kernel,
        out_shape=(
            jax.ShapeDtypeStruct((blocks, cols, size), bf16),
            jax.ShapeDtypeStruct((MAXS,), f32),
        ),
        in_specs=[vm, vm, vm],
        out_specs=(anywhere, pl.BlockSpec(memory_space=pltpu.SMEM)),
        scratch_shapes=[
            pltpu.VMEM((blocks, cols, size), bf16),
            pltpu.VMEM((2, size, size), bf16),
            pltpu.SemaphoreType.DMA((blocks,)),
        ],
        compiler_params=pltpu.CompilerParams(vmem_limit_bytes=28 << 20),
        name="apply_factors",
    )(packed, tops, gradients)


BLK = AXES[:3]


def per_device(ny, statistics, gradients, live_counts, slot_row, sweeps):
    matrices = statistics[0]
    live_counts, slot_row, sweeps, matrices = (
        pltpu.with_memory_space_constraint(value, pltpu.HBM)
        for value in (live_counts, slot_row, sweeps, matrices)
    )
    packed, offs, where_of = jacobi(
        live_counts, slot_row, sweeps, gradients.shape[1], matrices
    )
    pieces, tops = gather(where_of, packed, offs, ny)
    updates, off_max = apply(pieces, tops, jnp.swapaxes(gradients[0], 1, 2))
    return jnp.swapaxes(updates, 1, 2)[None], off_max


def solution(mesh):
    ny = mesh.shape["grp"]
    split_mesh = Mesh(mesh.devices.reshape(4, 4, 2, ny), AXES)
    return jax.shard_map(
        functools.partial(per_device, ny),
        mesh=split_mesh,
        in_specs=(
            P("grp", BLK, None, None),
            P("grp", None, None, BLK),
            P("grp", None),
            P("grp", None),
            P("grp", BLK),
        ),
        out_specs=(P("grp", None, None, BLK), P()),
        check_vma=False,
    )
```

```python
import functools
import jax
import jax.numpy as jnp
from jax import lax
from jax.experimental import pallas as pl
from jax.experimental.pallas import tpu as pltpu
from jax.sharding import Mesh
from jax.sharding import PartitionSpec as P

MAXS = 2
GW = 128
damping = 0.01
pairings = ((0, 1, 2, 3), (0, 2, 1, 3), (0, 3, 1, 2))
f32, bf16 = jnp.float32, jnp.bfloat16
TOL = 1e-6
EASY = 0.8
TILES = [(i, j) for i in range(4) for j in range(i, 4)]


def split(x):
    hi = x.astype(bf16)
    return hi, (x - hi.astype(f32)).astype(bf16)


def dot(a, b):
    return jnp.dot(a, b, preferred_element_type=f32)


def dot3(a, b):
    return dot(a[0], b[0]) + (dot(a[1], b[0]) + dot(a[0], b[1]))


def dot3_packed(a, b):
    left = jnp.concatenate([a[0], a[1]], axis=1)
    top = jnp.concatenate([b[0], b[1]], axis=1)
    low = jnp.concatenate([b[0], jnp.zeros_like(b[1])], axis=1)
    both = dot(left, jnp.concatenate([top, low], axis=0))
    return both[:, :GW] + both[:, GW:]


def two(a, b):
    return jnp.concatenate([a, b], axis=1)


def apart(pair):
    blank = jnp.zeros((GW, GW), pair.dtype)
    return jnp.concatenate([two(pair[:, :GW], blank), two(blank, pair[:, GW:])], axis=0)


def grp(member):
    return slice(member * GW, (member + 1) * GW)


def eye_mask(size):
    rows = lax.broadcasted_iota(jnp.int32, (size, size), 0)
    return rows == lax.broadcasted_iota(jnp.int32, (size, size), 1)


def inverse_rare(jobs, w_ref, b_ref, p_ref, peak):
    identity = eye_mask(GW).astype(f32)
    alpha = 2.0 / (2.0 + peak)
    for j in jobs:
        c = (1.0 - alpha) * identity - alpha * b_ref[j]
        p_ref[j] = c
        w_ref[j] = identity + c

    def more(r):
        for j in jobs:
            sp = split(p_ref[j])
            p = dot3(sp, sp)
            p_ref[j] = p
            t = w_ref[j]
            w_ref[j] = t + dot3(split(t), split(p))
        return r * r

    rho = peak / (2.0 + peak)
    lax.while_loop(lambda r: r > TOL, more, rho * rho)
    for j in jobs:
        w_ref[j] = alpha * w_ref[j]


def sweep_body(slots, m_ref, v_ref, w_ref, b_ref, p_ref):
    mask = eye_mask(GW)
    identity = mask.astype(f32)
    eye2 = two(identity, identity)

    def block(s, rows, cols):
        lines = [two(m_ref[s, grp(a), grp(cols[0])], m_ref[s, grp(a), grp(cols[1])]) for a in rows]
        return jnp.concatenate(lines, axis=0)

    def store(s, rows, cols, value):
        for i, a in enumerate(rows):
            for j, b in enumerate(cols):
                m_ref[s, grp(a), grp(b)] = value[grp(i), grp(j)]

    def settle(n, s, halves, turns, own):
        for h in range(2):
            r, rt = turns[n, h]
            store(s, halves[h], halves[h], dot3(rt, split(own[n, h])))
            cols = two(v_ref[s, :, grp(halves[h][0])], v_ref[s, :, grp(halves[h][1])])
            turned = dot3(split(cols), r)
            for i in range(2):
                v_ref[s, :, grp(halves[h][i])] = turned[:, grp(i)]

    last, diagonals, turns, own = None, {}, {}, {}
    for pairing in pairings:
        halves = (pairing[:2], pairing[2:])
        peak = None
        kept = {}
        for n, s in enumerate(slots):
            ang, mats = [], []
            for h, (a, b) in enumerate(halves):
                if last is None:
                    low = jnp.sum(jnp.where(mask, m_ref[s, grp(a), grp(a)], 0.0), axis=1, keepdims=True)
                    up = jnp.sum(jnp.where(mask, m_ref[s, grp(b), grp(b)], 0.0), axis=0, keepdims=True)
                else:
                    low = jnp.sum(jnp.where(mask, diagonals[n, a], 0.0), axis=1, keepdims=True)
                    up = diagonals[n, b]
                c = m_ref[s, grp(a), grp(b)]
                diff = up - low
                both = up + low
                one = c * diff / (diff * diff + 4.0 * c * c + damping * (both * both))
                sa, sat = split(one), split(one.T)
                bb = 0.25 * dot3_packed(sa, sat)
                b_ref[2 * n + h] = bb
                ang.append((sa, sat))
                mats.append(bb)
            bb = two(*mats)
            bound = jnp.max(jnp.sum(jnp.abs(bb), axis=0, keepdims=True), axis=1, keepdims=True)
            alpha = 2.0 / (2.0 + bound)
            c = (1.0 - alpha) * eye2 - alpha * bb
            cb = c.astype(bf16)
            p = dot(cb, apart(cb))
            t = eye2 + c
            w = alpha * (t + dot(t.astype(bf16), apart(p.astype(bf16))))
            done = two(*[
                dot3_packed(split(mats[h]), split(w[:, grp(h)])) for h in range(2)
            ])
            error = eye2 - w - done
            w = w + dot(w.astype(bf16), apart(error.astype(bf16)))
            for h in range(2):
                w_ref[2 * n + h] = w[:, grp(h)]
            kept[n] = ang
            peak = bound if peak is None else jnp.maximum(peak, bound)
            if last is not None:
                settle(n, s, last, turns, own)
        peak = jnp.max(peak)

        @pl.when(peak > EASY)
        def _():
            inverse_rare(range(2 * len(slots)), w_ref, b_ref, p_ref, peak)

        for n, s in enumerate(slots):
            for h, (sa, sat) in enumerate(kept[n]):
                w = w_ref[2 * n + h]
                x = dot3_packed(split(w), sa)
                sx = split(x)
                q = identity - 0.5 * dot3_packed(sat, sx)
                p = 2.0 * w - identity
                sp, sq, sxt = split(p), split(q), split(x.T)
                turns[n, h] = (
                    [jnp.concatenate([two(sp[i], sx[i]), two(-sxt[i], sq[i])], axis=0) for i in range(2)],
                    [jnp.concatenate([two(sp[i], -sx[i]), two(sxt[i], sq[i])], axis=0) for i in range(2)],
                )
        for n, s in enumerate(slots):
            (r0, rt0), (r1, _) = turns[n, 0], turns[n, 1]
            z = dot3(rt0, split(dot3(split(block(s, halves[0], halves[1])), r1)))
            for h, r in enumerate((r0, r1)):
                y = dot3(split(block(s, halves[h], halves[h])), r)
                own[n, h] = y
                full = r[0].astype(f32) + r[1].astype(f32)
                row = jnp.sum(full * y, axis=0, keepdims=True)
                for i in range(2):
                    diagonals[n, halves[h][i]] = row[:, grp(i)]
            store(s, halves[0], halves[1], z)
            store(s, halves[1], halves[0], z.T)
        last = halves
    for n, s in enumerate(slots):
        settle(n, s, last, turns, own)


def off_norm(matrix, mask):
    square = matrix * matrix
    off = jnp.sum(jnp.where(mask, 0.0, square))
    return jnp.sqrt(off / jnp.sum(square))


def finish(slots, m_ref, v_ref, f_ref, mask):
    dot = functools.partial(
        lax.dot_general, dimension_numbers=(((1,), (1,)), ((), ())), preferred_element_type=f32
    )
    for s in slots:
        diagonal = jnp.sum(jnp.where(mask, m_ref[s], 0.0), axis=0, keepdims=True)
        eighth = jnp.sqrt(lax.rsqrt(jnp.sqrt(diagonal)))
        hi, lo = split(v_ref[s] * eighth)
        for i in range(4):
            ah, al, bh, bl = hi[grp(i)], lo[grp(i)], hi[i * GW :], lo[i * GW :]
            line = (dot(ah, bh) + (dot(al, bh) + dot(ah, bl))).astype(bf16)
            for j in range(i, 4):
                t = TILES.index((i, j))
                f_ref[s, grp(t), :] = line[:, grp(j - i)]


def note_off(off_ref, i, value):
    rows = lax.broadcasted_iota(jnp.int32, off_ref.shape, 0)
    off_ref[...] = jnp.where(rows == i, jnp.maximum(off_ref[...], value), off_ref[...])


def jacobi_kernel(
    live_any, row_any, sweeps_any, stats_ref,
    f_ref, off_ref, place_ref, m_ref, v_ref, w_ref, b_ref, p_ref, live_s, row_s, sweeps_s, sem,
):
    small = [
        pltpu.make_async_copy(src, dst, sem.at[2 + i])
        for i, (src, dst) in enumerate(
            ((live_any, live_s), (row_any, row_s), (sweeps_any, sweeps_s))
        )
    ]
    def load(s):
        return pltpu.make_async_copy(stats_ref.at[s], m_ref.at[s], sem.at[s])

    for copy in small:
        copy.start()
    for s in range(2):
        load(s).start()
    for copy in small:
        copy.wait()
    live_ref, row_ref, sweeps_ref = live_s.at[0], row_s.at[0], sweeps_s.at[0]
    size = stats_ref.shape[1]
    devices = live_ref.shape[0]
    mask = eye_mask(size)
    rank = (lax.axis_index("blk_0") * 4 + lax.axis_index("blk_1")) * 2 + lax.axis_index("blk_2")
    own = live_ref[rank]
    n0 = jnp.where(own > 0, sweeps_ref[0], 0)
    n1 = jnp.where(own > 1, sweeps_ref[1], 0)

    spare = place_ref.shape[0] - 1

    def note_place(d, carry):
        base = lax.rem(d, 2) * devices + (d // 2) * 2
        for i in range(2):
            place_ref[jnp.where(i < live_ref[d], row_ref[2 * d + i], spare)] = base + i
        return carry

    lax.fori_loop(0, devices, note_place, 0, unroll=4)
    off_ref[...] = jnp.zeros_like(off_ref)
    scratch = (m_ref, v_ref, w_ref, b_ref, p_ref)

    for s, n in enumerate((n0, n1)):

        @pl.when(n > 0)
        def _(s=s):
            v_ref[s] = mask.astype(f32)

    for s in range(2):
        load(s).wait()

    def sweep(i, carry):
        a0, a1 = n0 > i, n1 > i
        slot = jnp.where(a0, 0, 1)

        @pl.when(a0 & a1)
        def _():
            sweep_body((0, 1), *scratch)
            for s in range(2):
                note_off(off_ref, i, off_norm(m_ref[s], eye_mask(size)))

        @pl.when(a0 != a1)
        def _():
            sweep_body((slot,), *scratch)
            note_off(off_ref, i, off_norm(m_ref[slot], eye_mask(size)))

        return carry

    lax.fori_loop(0, MAXS, sweep, 0)

    @pl.when(n0 > 0)
    def _():
        finish((0,), m_ref, v_ref, f_ref, mask)

    @pl.when(n1 > 0)
    def _():
        finish((1,), m_ref, v_ref, f_ref, mask)


def jacobi(live, slot_row, sweeps, blocks, stats):
    slots, size, _ = stats.shape
    vm = pl.BlockSpec(memory_space=pltpu.VMEM)
    sm = pl.BlockSpec(memory_space=pltpu.SMEM)
    return pl.pallas_call(
        jacobi_kernel,
        out_shape=(
            jax.ShapeDtypeStruct((slots, len(TILES) * GW, GW), bf16),
            jax.ShapeDtypeStruct((8, GW), f32),
            jax.ShapeDtypeStruct((blocks + 8,), jnp.int32),
        ),
        in_specs=[pl.BlockSpec(memory_space=pltpu.HBM)] * 4,
        out_specs=(vm, vm, sm),
        scratch_shapes=[
            pltpu.VMEM((slots, size, size), f32),
            pltpu.VMEM((slots, size, size), f32),
            pltpu.VMEM((2 * slots, GW, GW), f32),
            pltpu.VMEM((2 * slots, GW, GW), f32),
            pltpu.VMEM((2 * slots, GW, GW), f32),
            pltpu.SMEM(live.shape, jnp.int32),
            pltpu.SMEM(slot_row.shape, jnp.int32),
            pltpu.SMEM(sweeps.shape, jnp.int32),
            pltpu.SemaphoreType.DMA((5,)),
        ],
        cost_estimate=pl.CostEstimate(flops=20 * 10**9, bytes_accessed=1 << 20, transcendentals=0),
        compiler_params=pltpu.CompilerParams(vmem_limit_bytes=24 << 20),
        name="jacobi",
    )(live, slot_row, sweeps, stats)


AXES = ("blk_0", "blk_1", "blk_2", "grp")
CHUNKS = 4
WIDE = 8 // CHUNKS
MESH_ID = pl.DeviceIdType.MESH


STEPS = sorted(
    ((a, b) for a in range(4) for b in range(4) if a or b),
    key=lambda ab: -(min(ab[0], 4 - ab[0]) + min(ab[1], 4 - ab[1])),
)


def gather_kernel(ny, idx_ref, f_ref, off_ref, g, omax_ref,
                  spread, offs, ostage,
                  s1, r1, s2, r2, sa, ra, sb, rb, sc, rc, sd, rd, se, re,
                  so, ro, sp, rp, sq, rq):
    x, z, e, y = [lax.axis_index(a) for a in AXES]
    chip = x * 4 + z
    rows = f_ref.shape[1] // 16

    def ident(c, core, yy):
        return (c // 4, lax.rem(c, 4), core, yy)

    def remote(src, dst, send, recv, dev):
        return pltpu.make_async_remote_copy(
            src_ref=src, dst_ref=dst, send_sem=send, recv_sem=recv,
            device_id=dev, device_id_type=MESH_ID,
        )

    twin = ident(chip, 1 - e, y)

    def ahead(d):
        a, b = STEPS[d - 1]
        return lax.rem(x + a, 4) * 4 + lax.rem(z + b, 4)

    def behind(d):
        a, b = STEPS[d - 1]
        return lax.rem(x + 4 - a, 4) * 4 + lax.rem(z + 4 - b, 4)

    def peer(d):
        return ident(ahead(d), e, y)

    def level(d):
        return ident(chip, e, lax.rem(y + d, ny))

    barrier = pltpu.get_barrier_semaphore()

    for d in range(1, 16):
        pl.semaphore_signal(barrier, inc=1, device_id=peer(d), device_id_type=MESH_ID)
    for d in range(1, ny):
        pl.semaphore_signal(barrier, inc=1, device_id=level(d), device_id_type=MESH_ID)
    pl.semaphore_signal(barrier, inc=1, device_id=twin, device_id_type=MESH_ID)
    pl.semaphore_wait(barrier, 15 + (ny - 1) + 1)

    def my_rows(c):
        return f_ref.at[:, pl.ds(pl.multiple_of(c * rows, 16), rows), :]

    def spread_copy(d):
        return remote(my_rows(ahead(d)), spread.at[e, chip], s1.at[d], r1.at[d], peer(d))

    def pass_copy(d):
        source = behind(d)
        return remote(spread.at[e, source], spread.at[e, source], s2.at[d], r2.at[d], twin)

    def own_copy():
        return remote(my_rows(chip), spread.at[e, chip], s2.at[0], r2.at[0], twin)

    def off_copy(d):
        return remote(off_ref, offs.at[d], so.at[d], ro.at[d], peer(d))

    for d in range(1, 16):
        spread_copy(d).start()
    own_copy().start()
    spread[e, chip] = f_ref[:, pl.ds(pl.multiple_of(chip * rows, 16), rows), :]
    offs[0] = off_ref[...]
    for d in range(1, 16):
        spread_copy(d).wait_recv()
        pass_copy(d).start()
    for d in range(16):
        source = behind(d) if d else chip
        remote(
            spread.at[1 - e, source], spread.at[1 - e, source], s2.at[d], r2.at[d], twin
        ).wait_recv()

    for q in range(CHUNKS):
        for b in range(WIDE):
            k = WIDE * (2 * q + e) + b
            j = idx_ref[k]
            g[chip, k] = spread[j // 32, lax.rem(j, 32) // 2, lax.rem(j, 2)]

    pos1 = jnp.where(e == 0, x, z)
    pos2 = jnp.where(e == 0, z, x)

    def at(p1, p2):
        p1, p2 = lax.rem(p1, 4), lax.rem(p2, 4)
        return jnp.where(e == 0, p1 * 4 + p2, p2 * 4 + p1)

    def pair(c, q):
        return g.at[c, pl.ds(WIDE * (2 * q + e), WIDE)]

    def single(c, q, b):
        return g.at[c, pl.ds(WIDE * (2 * q + e) + WIDE // 2 * b, WIDE // 2)]

    def first(q, w):
        dev = ident(at(pos1 + 1 + 2 * w, pos2), e, y)
        return remote(pair(chip, q), pair(chip, q), sa.at[q, w], ra.at[q, w], dev)

    def first_in(q, w):
        c = at(pos1 + 3 - 2 * w, pos2)
        return remote(pair(c, q), pair(c, q), sa.at[q, w], ra.at[q, w], twin)

    def second(q, w):
        c = at(pos1 + 3 - 2 * w, pos2)
        dev = ident(at(pos1 + 1 + 2 * w, pos2), e, y)
        return remote(single(c, q, w), single(c, q, w), sb.at[q, w], rb.at[q, w], dev)

    def second_in(q, w):
        c = at(pos1 + 2, pos2)
        return remote(single(c, q, w), single(c, q, w), sb.at[q, w], rb.at[q, w], twin)

    def third(q, o, w):
        c = at(pos1 + o, pos2)
        dev = ident(at(pos1, pos2 + 1 + 2 * w), e, y)
        return remote(pair(c, q), pair(c, q), sc.at[q, o, w], rc.at[q, o, w], dev)

    def third_in(q, o, w):
        c = at(pos1 + o, pos2 + 3 - 2 * w)
        return remote(pair(c, q), pair(c, q), sc.at[q, o, w], rc.at[q, o, w], twin)

    def fourth(q, o, w):
        c = at(pos1 + o, pos2 + 3 - 2 * w)
        dev = ident(at(pos1, pos2 + 1 + 2 * w), e, y)
        return remote(single(c, q, w), single(c, q, w), sd.at[q, o, w], rd.at[q, o, w], dev)

    def fourth_in(q, o, w):
        c = at(pos1 + o, pos2 + 2)
        return remote(single(c, q, w), single(c, q, w), sd.at[q, o, w], rd.at[q, o, w], twin)

    def across(q, core):
        part = g.at[:, pl.ds(WIDE * (2 * q + core), WIDE)]
        return remote(part, part, se.at[q], re.at[q], twin)

    def wave0(q, carry):
        for w in range(2):
            first(q, w).start()
            third(q, 0, w).start()
        return carry

    def wave1(q, carry):
        for w in range(2):
            first_in(q, w).wait_recv()
            second(q, w).start()
        for w in range(2):
            third(q, 1, w).start()
            third(q, 3, w).start()
        for w in range(2):
            third_in(q, 0, w).wait_recv()
            fourth(q, 0, w).start()
        return carry

    def wave2(q, carry):
        for w in range(2):
            second_in(q, w).wait_recv()
        for w in range(2):
            third(q, 2, w).start()
        for o in (1, 3):
            for w in range(2):
                third_in(q, o, w).wait_recv()
                fourth(q, o, w).start()
        return carry

    def wave3(q, carry):
        for w in range(2):
            third_in(q, 2, w).wait_recv()
            fourth(q, 2, w).start()
        return carry

    def wave4(q, carry):
        for o in range(4):
            for w in range(2):
                fourth_in(q, o, w).wait_recv()
        across(q, e).start()
        return carry

    def wave5(q, carry):
        across(q, 1 - e).wait_recv()
        return carry

    def level_copy(d):
        return remote(ostage.at[0], ostage.at[d], sp.at[d], rp.at[d], level(d))

    def core_copy():
        return remote(ostage.at[ny], ostage.at[ny + 1], sq, rq, twin)

    lax.fori_loop(0, CHUNKS, wave0, 0)
    for d in range(1, 16):
        off_copy(d).start()
    lax.fori_loop(0, CHUNKS, wave1, 0)
    top = offs[0]
    for d in range(1, 16):
        off_copy(d).wait_recv()
        top = jnp.maximum(top, offs[d])
    ostage[0] = top
    lax.fori_loop(0, CHUNKS, wave2, 0)
    for d in range(1, ny):
        level_copy(d).start()
    lax.fori_loop(0, CHUNKS, wave3, 0)
    for d in range(1, ny):
        level_copy(d).wait_recv()
        top = jnp.maximum(top, ostage[d])
    ostage[ny] = top
    lax.fori_loop(0, CHUNKS - 1, wave4, 0)
    core_copy().start()
    wave4(CHUNKS - 1, 0)
    lax.fori_loop(0, CHUNKS, wave5, 0)
    core_copy().wait_recv()
    omax_ref[...] = jnp.maximum(top, ostage[ny + 1])

    own_copy().wait_send()

    for d in range(1, 16):
        spread_copy(d).wait_send()
        pass_copy(d).wait_send()
        off_copy(d).wait_send()
    for d in range(1, ny):
        level_copy(d).wait_send()
    core_copy().wait_send()

    def drain_chunk(q, carry):
        for w in range(2):
            first(q, w).wait_send()
            second(q, w).wait_send()
            for o in range(4):
                third(q, o, w).wait_send()
                fourth(q, o, w).wait_send()
        across(q, e).wait_send()
        return carry

    lax.fori_loop(0, CHUNKS, drain_chunk, 0)


def gather(idx, blocks, packed, offs, ny):
    slots, length, width = packed.shape
    rows = length // 16
    vm = pl.BlockSpec(memory_space=pltpu.VMEM)
    dma = pltpu.SemaphoreType.DMA
    n = CHUNKS
    return pl.pallas_call(
        functools.partial(gather_kernel, ny),
        out_shape=(
            jax.ShapeDtypeStruct((16, blocks, rows, width), bf16),
            jax.ShapeDtypeStruct(offs.shape, f32),
        ),
        in_specs=[pl.BlockSpec(memory_space=pltpu.SMEM), vm, vm],
        out_specs=(vm, vm),
        scratch_shapes=[
            pltpu.VMEM((2, 16, slots, rows, width), bf16),
            pltpu.VMEM((16,) + offs.shape, f32),
            pltpu.VMEM((ny + 2,) + offs.shape, f32),
            dma((16,)), dma((16,)), dma((16,)), dma((16,)),
            dma((n, 2)), dma((n, 2)), dma((n, 2)), dma((n, 2)),
            dma((n, 4, 2)), dma((n, 4, 2)), dma((n, 4, 2)), dma((n, 4, 2)),
            dma((n,)), dma((n,)),
            dma((16,)), dma((16,)), dma((ny,)), dma((ny,)), dma, dma,
        ],
        compiler_params=pltpu.CompilerParams(
            collective_id=0, has_side_effects=True, vmem_limit_bytes=16 << 20
        ),
        cost_estimate=pl.CostEstimate(flops=20 * 10**9, bytes_accessed=1 << 20, transcendentals=0),
        name="gather_factors",
    )(idx, packed, offs)


def apply_kernel(p_ref, o_ref, g_ref, u_any, tops_ref, u_ref, f_ref, out_sem):
    blocks = g_ref.shape[0]
    rows = p_ref.shape[2]

    def save(k):
        return pltpu.make_async_copy(u_ref.at[k], u_any.at[k], out_sem.at[k])

    for i in range(MAXS):
        tops_ref[i] = jnp.max(o_ref[i : i + 1, :])

    def assemble(k, slot):
        packed = p_ref[:, k].reshape(p_ref.shape[0] * rows, GW)
        for t, (i, j) in enumerate(TILES):
            tile = packed[grp(t)]
            f_ref[slot, grp(i), grp(j)] = tile
            if i != j:
                f_ref[slot, grp(j), grp(i)] = tile.T

    def turn(k, slot):
        u_ref[k] = dot(g_ref[k], f_ref[slot]).astype(bf16)

    assemble(0, 0)

    def step(n, carry):
        k = 2 * n
        assemble(k + 1, 1)
        turn(k, 0)
        assemble(jnp.minimum(k + 2, blocks - 1), 0)
        turn(k + 1, 1)
        save(k).start()
        save(k + 1).start()
        return carry

    lax.fori_loop(0, blocks // 2, step, 0)
    for k in range(blocks):
        save(k).wait()


def apply(packed, tops, gradients):
    blocks, cols, size = gradients.shape
    anywhere = pl.BlockSpec(memory_space=pl.ANY)
    vm = pl.BlockSpec(memory_space=pltpu.VMEM)
    return pl.pallas_call(
        apply_kernel,
        out_shape=(
            jax.ShapeDtypeStruct((blocks, cols, size), bf16),
            jax.ShapeDtypeStruct((MAXS,), f32),
        ),
        in_specs=[vm, vm, vm],
        out_specs=(anywhere, pl.BlockSpec(memory_space=pltpu.SMEM)),
        scratch_shapes=[
            pltpu.VMEM((blocks, cols, size), bf16),
            pltpu.VMEM((2, size, size), bf16),
            pltpu.SemaphoreType.DMA((blocks,)),
        ],
        compiler_params=pltpu.CompilerParams(vmem_limit_bytes=28 << 20),
        name="apply_factors",
    )(packed, tops, gradients)


BLK = AXES[:3]


def per_device(ny, statistics, gradients, live_counts, slot_row, sweeps):
    matrices = statistics[0]
    live_counts, slot_row, sweeps, matrices = (
        pltpu.with_memory_space_constraint(value, pltpu.HBM)
        for value in (live_counts, slot_row, sweeps, matrices)
    )
    packed, offs, where_of = jacobi(
        live_counts, slot_row, sweeps, gradients.shape[1], matrices
    )
    pieces, tops = gather(where_of, gradients.shape[1], packed, offs, ny)
    updates, off_max = apply(pieces, tops, jnp.swapaxes(gradients[0], 1, 2))
    return jnp.swapaxes(updates, 1, 2)[None], off_max


def solution(mesh):
    ny = mesh.shape["grp"]
    split_mesh = Mesh(mesh.devices.reshape(4, 4, 2, ny), AXES)
    return jax.shard_map(
        functools.partial(per_device, ny),
        mesh=split_mesh,
        in_specs=(
            P("grp", BLK, None, None),
            P("grp", None, None, BLK),
            P("grp", None),
            P("grp", None),
            P("grp", BLK),
        ),
        out_specs=(P("grp", None, None, BLK), P()),
        check_vma=False,
    )
```

```python
import functools
import jax
import jax.numpy as jnp
from jax import lax
from jax.experimental import pallas as pl
from jax.experimental.pallas import tpu as pltpu
from jax.sharding import Mesh
from jax.sharding import PartitionSpec as P

MAXS = 2
GW = 128
damping = 0.01
pairings = ((0, 1, 2, 3), (0, 2, 1, 3), (0, 3, 1, 2))
f32, bf16 = jnp.float32, jnp.bfloat16
TOL = 1e-6
EASY = 0.8
TILES = [(i, j) for i in range(4) for j in range(i, 4)]


def split(x):
    hi = x.astype(bf16)
    return hi, (x - hi.astype(f32)).astype(bf16)


def dot(a, b):
    return jnp.dot(a, b, preferred_element_type=f32)


def dot3(a, b):
    return dot(a[0], b[0]) + (dot(a[1], b[0]) + dot(a[0], b[1]))


def dot3_packed(a, b):
    left = jnp.concatenate([a[0], a[1]], axis=1)
    top = jnp.concatenate([b[0], b[1]], axis=1)
    low = jnp.concatenate([b[0], jnp.zeros_like(b[1])], axis=1)
    both = dot(left, jnp.concatenate([top, low], axis=0))
    return both[:, :GW] + both[:, GW:]


def two(a, b):
    return jnp.concatenate([a, b], axis=1)


def apart(pair):
    blank = jnp.zeros((GW, GW), pair.dtype)
    return jnp.concatenate([two(pair[:, :GW], blank), two(blank, pair[:, GW:])], axis=0)


def grp(member):
    return slice(member * GW, (member + 1) * GW)


def eye_mask(size):
    rows = lax.broadcasted_iota(jnp.int32, (size, size), 0)
    return rows == lax.broadcasted_iota(jnp.int32, (size, size), 1)


def inverse_rare(jobs, w_ref, b_ref, p_ref, peak):
    identity = eye_mask(GW).astype(f32)
    alpha = 2.0 / (2.0 + peak)
    for j in jobs:
        c = (1.0 - alpha) * identity - alpha * b_ref[j]
        p_ref[j] = c
        w_ref[j] = identity + c

    def more(r):
        for j in jobs:
            sp = split(p_ref[j])
            p = dot3(sp, sp)
            p_ref[j] = p
            t = w_ref[j]
            w_ref[j] = t + dot3(split(t), split(p))
        return r * r

    rho = peak / (2.0 + peak)
    lax.while_loop(lambda r: r > TOL, more, rho * rho)
    for j in jobs:
        w_ref[j] = alpha * w_ref[j]


def sweep_body(slots, m_ref, v_ref, w_ref, b_ref, p_ref):
    mask = eye_mask(GW)
    identity = mask.astype(f32)
    eye2 = two(identity, identity)

    def block(s, rows, cols):
        lines = [two(m_ref[s, grp(a), grp(cols[0])], m_ref[s, grp(a), grp(cols[1])]) for a in rows]
        return jnp.concatenate(lines, axis=0)

    def store(s, rows, cols, value):
        for i, a in enumerate(rows):
            for j, b in enumerate(cols):
                m_ref[s, grp(a), grp(b)] = value[grp(i), grp(j)]

    def settle(n, s, halves, turns, own):
        for h in range(2):
            r, rt = turns[n, h]
            store(s, halves[h], halves[h], dot3(rt, split(own[n, h])))
            cols = two(v_ref[s, :, grp(halves[h][0])], v_ref[s, :, grp(halves[h][1])])
            turned = dot3(split(cols), r)
            for i in range(2):
                v_ref[s, :, grp(halves[h][i])] = turned[:, grp(i)]

    last, diagonals, turns, own = None, {}, {}, {}
    for pairing in pairings:
        halves = (pairing[:2], pairing[2:])
        peak = None
        kept = {}
        for n, s in enumerate(slots):
            ang, mats = [], []
            for h, (a, b) in enumerate(halves):
                if last is None:
                    low = jnp.sum(jnp.where(mask, m_ref[s, grp(a), grp(a)], 0.0), axis=1, keepdims=True)
                    up = jnp.sum(jnp.where(mask, m_ref[s, grp(b), grp(b)], 0.0), axis=0, keepdims=True)
                else:
                    low = jnp.sum(jnp.where(mask, diagonals[n, a], 0.0), axis=1, keepdims=True)
                    up = diagonals[n, b]
                c = m_ref[s, grp(a), grp(b)]
                diff = up - low
                both = up + low
                one = c * diff / (diff * diff + 4.0 * c * c + damping * (both * both))
                sa, sat = split(one), split(one.T)
                bb = 0.25 * dot3_packed(sa, sat)
                b_ref[2 * n + h] = bb
                ang.append((sa, sat))
                mats.append(bb)
            bb = two(*mats)
            bound = jnp.max(jnp.sum(jnp.abs(bb), axis=0, keepdims=True), axis=1, keepdims=True)
            alpha = 2.0 / (2.0 + bound)
            c = (1.0 - alpha) * eye2 - alpha * bb
            cb = c.astype(bf16)
            p = dot(cb, apart(cb))
            t = eye2 + c
            w = alpha * (t + dot(t.astype(bf16), apart(p.astype(bf16))))
            done = two(*[
                dot3_packed(split(mats[h]), split(w[:, grp(h)])) for h in range(2)
            ])
            error = eye2 - w - done
            w = w + dot(w.astype(bf16), apart(error.astype(bf16)))
            for h in range(2):
                w_ref[2 * n + h] = w[:, grp(h)]
            kept[n] = ang
            peak = bound if peak is None else jnp.maximum(peak, bound)
            if last is not None:
                settle(n, s, last, turns, own)
        peak = jnp.max(peak)

        @pl.when(peak > EASY)
        def _():
            inverse_rare(range(2 * len(slots)), w_ref, b_ref, p_ref, peak)

        for n, s in enumerate(slots):
            for h, (sa, sat) in enumerate(kept[n]):
                w = w_ref[2 * n + h]
                x = dot3_packed(split(w), sa)
                sx = split(x)
                q = identity - 0.5 * dot3_packed(sat, sx)
                p = 2.0 * w - identity
                sp, sq, sxt = split(p), split(q), split(x.T)
                turns[n, h] = (
                    [jnp.concatenate([two(sp[i], sx[i]), two(-sxt[i], sq[i])], axis=0) for i in range(2)],
                    [jnp.concatenate([two(sp[i], -sx[i]), two(sxt[i], sq[i])], axis=0) for i in range(2)],
                )
        for n, s in enumerate(slots):
            (r0, rt0), (r1, _) = turns[n, 0], turns[n, 1]
            z = dot3(rt0, split(dot3(split(block(s, halves[0], halves[1])), r1)))
            for h, r in enumerate((r0, r1)):
                y = dot3(split(block(s, halves[h], halves[h])), r)
                own[n, h] = y
                full = r[0].astype(f32) + r[1].astype(f32)
                row = jnp.sum(full * y, axis=0, keepdims=True)
                for i in range(2):
                    diagonals[n, halves[h][i]] = row[:, grp(i)]
            store(s, halves[0], halves[1], z)
            store(s, halves[1], halves[0], z.T)
        last = halves
    for n, s in enumerate(slots):
        settle(n, s, last, turns, own)


def off_norm(matrix, mask):
    square = matrix * matrix
    off = jnp.sum(jnp.where(mask, 0.0, square))
    return jnp.sqrt(off / jnp.sum(square))


def finish(slots, m_ref, v_ref, f_ref, mask):
    dot = functools.partial(
        lax.dot_general, dimension_numbers=(((1,), (1,)), ((), ())), preferred_element_type=f32
    )
    for s in slots:
        diagonal = jnp.sum(jnp.where(mask, m_ref[s], 0.0), axis=0, keepdims=True)
        eighth = jnp.sqrt(lax.rsqrt(jnp.sqrt(diagonal)))
        hi, lo = split(v_ref[s] * eighth)
        for i in range(4):
            ah, al, bh, bl = hi[grp(i)], lo[grp(i)], hi[i * GW :], lo[i * GW :]
            line = (dot(ah, bh) + (dot(al, bh) + dot(ah, bl))).astype(bf16)
            for j in range(i, 4):
                t = TILES.index((i, j))
                f_ref[s, grp(t), :] = line[:, grp(j - i)]


def note_off(off_ref, i, value):
    rows = lax.broadcasted_iota(jnp.int32, off_ref.shape, 0)
    off_ref[...] = jnp.where(rows == i, jnp.maximum(off_ref[...], value), off_ref[...])


def jacobi_kernel(
    live_any, row_any, sweeps_any, stats_ref,
    f_ref, off_ref, place_ref, m_ref, v_ref, w_ref, b_ref, p_ref, live_s, row_s, sweeps_s, sem,
):
    small = [
        pltpu.make_async_copy(src, dst, sem.at[2 + i])
        for i, (src, dst) in enumerate(
            ((live_any, live_s), (row_any, row_s), (sweeps_any, sweeps_s))
        )
    ]
    def load(s):
        return pltpu.make_async_copy(stats_ref.at[s], m_ref.at[s], sem.at[s])

    for copy in small:
        copy.start()
    for s in range(2):
        load(s).start()
    for copy in small:
        copy.wait()
    live_ref, row_ref, sweeps_ref = live_s.at[0], row_s.at[0], sweeps_s.at[0]
    size = stats_ref.shape[1]
    devices = live_ref.shape[0]
    mask = eye_mask(size)
    rank = (lax.axis_index("blk_0") * 4 + lax.axis_index("blk_1")) * 2 + lax.axis_index("blk_2")
    own = live_ref[rank]
    n0 = jnp.where(own > 0, sweeps_ref[0], 0)
    n1 = jnp.where(own > 1, sweeps_ref[1], 0)

    spare = place_ref.shape[0] - 1

    def note_place(d, carry):
        base = lax.rem(d, 2) * devices + (d // 2) * 2
        for i in range(2):
            place_ref[jnp.where(i < live_ref[d], row_ref[2 * d + i], spare)] = base + i
        return carry

    lax.fori_loop(0, devices, note_place, 0, unroll=4)
    off_ref[...] = jnp.zeros_like(off_ref)
    scratch = (m_ref, v_ref, w_ref, b_ref, p_ref)

    for s, n in enumerate((n0, n1)):

        @pl.when(n > 0)
        def _(s=s):
            v_ref[s] = mask.astype(f32)

    for s in range(2):
        load(s).wait()

    def sweep(i, carry):
        a0, a1 = n0 > i, n1 > i
        slot = jnp.where(a0, 0, 1)

        @pl.when(a0 & a1)
        def _():
            sweep_body((0, 1), *scratch)
            for s in range(2):
                note_off(off_ref, i, off_norm(m_ref[s], eye_mask(size)))

        @pl.when(a0 != a1)
        def _():
            sweep_body((slot,), *scratch)
            note_off(off_ref, i, off_norm(m_ref[slot], eye_mask(size)))

        return carry

    lax.fori_loop(0, MAXS, sweep, 0)

    @pl.when((n0 > 0) & (n1 == 0))
    def _():
        finish((0,), m_ref, v_ref, f_ref, mask)

    @pl.when(n1 > 0)
    def _():
        finish((0, 1), m_ref, v_ref, f_ref, mask)


def jacobi(live, slot_row, sweeps, blocks, stats):
    slots, size, _ = stats.shape
    vm = pl.BlockSpec(memory_space=pltpu.VMEM)
    sm = pl.BlockSpec(memory_space=pltpu.SMEM)
    return pl.pallas_call(
        jacobi_kernel,
        out_shape=(
            jax.ShapeDtypeStruct((slots, len(TILES) * GW, GW), bf16),
            jax.ShapeDtypeStruct((8, GW), f32),
            jax.ShapeDtypeStruct((blocks + 8,), jnp.int32),
        ),
        in_specs=[pl.BlockSpec(memory_space=pltpu.HBM)] * 4,
        out_specs=(vm, vm, sm),
        scratch_shapes=[
            pltpu.VMEM((slots, size, size), f32),
            pltpu.VMEM((slots, size, size), f32),
            pltpu.VMEM((2 * slots, GW, GW), f32),
            pltpu.VMEM((2 * slots, GW, GW), f32),
            pltpu.VMEM((2 * slots, GW, GW), f32),
            pltpu.SMEM(live.shape, jnp.int32),
            pltpu.SMEM(slot_row.shape, jnp.int32),
            pltpu.SMEM(sweeps.shape, jnp.int32),
            pltpu.SemaphoreType.DMA((5,)),
        ],
        cost_estimate=pl.CostEstimate(flops=20 * 10**9, bytes_accessed=1 << 20, transcendentals=0),
        compiler_params=pltpu.CompilerParams(vmem_limit_bytes=24 << 20),
        name="jacobi",
    )(live, slot_row, sweeps, stats)


AXES = ("blk_0", "blk_1", "blk_2", "grp")
CHUNKS = 4
WIDE = 8 // CHUNKS
MESH_ID = pl.DeviceIdType.MESH


STEPS = sorted(
    ((a, b) for a in range(4) for b in range(4) if a or b),
    key=lambda ab: -(min(ab[0], 4 - ab[0]) + min(ab[1], 4 - ab[1])),
)


def gather_kernel(ny, idx_ref, f_ref, off_ref, g, omax_ref,
                  spread, offs, ostage,
                  s1, r1, s2, r2, sa, ra, sb, rb, sc, rc, sd, rd, se, re,
                  so, ro, sp, rp, sq, rq):
    x, z, e, y = [lax.axis_index(a) for a in AXES]
    chip = x * 4 + z
    rows = f_ref.shape[1] // 16

    def ident(c, core, yy):
        return (c // 4, lax.rem(c, 4), core, yy)

    def remote(src, dst, send, recv, dev):
        return pltpu.make_async_remote_copy(
            src_ref=src, dst_ref=dst, send_sem=send, recv_sem=recv,
            device_id=dev, device_id_type=MESH_ID,
        )

    twin = ident(chip, 1 - e, y)

    def ahead(d):
        a, b = STEPS[d - 1]
        return lax.rem(x + a, 4) * 4 + lax.rem(z + b, 4)

    def behind(d):
        a, b = STEPS[d - 1]
        return lax.rem(x + 4 - a, 4) * 4 + lax.rem(z + 4 - b, 4)

    def peer(d):
        return ident(ahead(d), e, y)

    def level(d):
        return ident(chip, e, lax.rem(y + d, ny))

    barrier = pltpu.get_barrier_semaphore()

    for d in range(1, 16):
        pl.semaphore_signal(barrier, inc=1, device_id=peer(d), device_id_type=MESH_ID)
    for d in range(1, ny):
        pl.semaphore_signal(barrier, inc=1, device_id=level(d), device_id_type=MESH_ID)
    pl.semaphore_signal(barrier, inc=1, device_id=twin, device_id_type=MESH_ID)
    pl.semaphore_wait(barrier, 15 + (ny - 1) + 1)

    def my_rows(c):
        return f_ref.at[:, pl.ds(pl.multiple_of(c * rows, 16), rows), :]

    def spread_copy(d):
        return remote(my_rows(ahead(d)), spread.at[e, chip], s1.at[d], r1.at[d], peer(d))

    def pass_copy(d):
        source = behind(d)
        return remote(spread.at[e, source], spread.at[e, source], s2.at[d], r2.at[d], twin)

    def own_copy():
        return remote(my_rows(chip), spread.at[e, chip], s2.at[0], r2.at[0], twin)

    def off_copy(d):
        return remote(off_ref, offs.at[d], so.at[d], ro.at[d], peer(d))

    for d in range(1, 16):
        spread_copy(d).start()
    own_copy().start()
    spread[e, chip] = f_ref[:, pl.ds(pl.multiple_of(chip * rows, 16), rows), :]
    offs[0] = off_ref[...]
    for d in range(1, 16):
        spread_copy(d).wait_recv()
        pass_copy(d).start()
    for d in range(16):
        source = behind(d) if d else chip
        remote(
            spread.at[1 - e, source], spread.at[1 - e, source], s2.at[d], r2.at[d], twin
        ).wait_recv()

    for q in range(CHUNKS):
        for b in range(WIDE):
            k = WIDE * (2 * q + e) + b
            j = idx_ref[k]
            g[chip, k] = spread[j // 32, lax.rem(j, 32) // 2, lax.rem(j, 2)]

    pos1 = jnp.where(e == 0, x, z)
    pos2 = jnp.where(e == 0, z, x)

    def at(p1, p2):
        p1, p2 = lax.rem(p1, 4), lax.rem(p2, 4)
        return jnp.where(e == 0, p1 * 4 + p2, p2 * 4 + p1)

    def pair(c, q):
        return g.at[c, pl.ds(WIDE * (2 * q + e), WIDE)]

    def single(c, q, b):
        return g.at[c, pl.ds(WIDE * (2 * q + e) + WIDE // 2 * b, WIDE // 2)]

    def first(q, w):
        dev = ident(at(pos1 + 1 + 2 * w, pos2), e, y)
        return remote(pair(chip, q), pair(chip, q), sa.at[q, w], ra.at[q, w], dev)

    def first_in(q, w):
        c = at(pos1 + 3 - 2 * w, pos2)
        return remote(pair(c, q), pair(c, q), sa.at[q, w], ra.at[q, w], twin)

    def second(q, w):
        c = at(pos1 + 3 - 2 * w, pos2)
        dev = ident(at(pos1 + 1 + 2 * w, pos2), e, y)
        return remote(single(c, q, w), single(c, q, w), sb.at[q, w], rb.at[q, w], dev)

    def second_in(q, w):
        c = at(pos1 + 2, pos2)
        return remote(single(c, q, w), single(c, q, w), sb.at[q, w], rb.at[q, w], twin)

    def third(q, o, w):
        c = at(pos1 + o, pos2)
        dev = ident(at(pos1, pos2 + 1 + 2 * w), e, y)
        return remote(pair(c, q), pair(c, q), sc.at[q, o, w], rc.at[q, o, w], dev)

    def third_in(q, o, w):
        c = at(pos1 + o, pos2 + 3 - 2 * w)
        return remote(pair(c, q), pair(c, q), sc.at[q, o, w], rc.at[q, o, w], twin)

    def fourth(q, o, w):
        c = at(pos1 + o, pos2 + 3 - 2 * w)
        dev = ident(at(pos1, pos2 + 1 + 2 * w), e, y)
        return remote(single(c, q, w), single(c, q, w), sd.at[q, o, w], rd.at[q, o, w], dev)

    def fourth_in(q, o, w):
        c = at(pos1 + o, pos2 + 2)
        return remote(single(c, q, w), single(c, q, w), sd.at[q, o, w], rd.at[q, o, w], twin)

    def across(q, core):
        part = g.at[:, pl.ds(WIDE * (2 * q + core), WIDE)]
        return remote(part, part, se.at[q], re.at[q], twin)

    def wave0(q, carry):
        for w in range(2):
            first(q, w).start()
            third(q, 0, w).start()
        return carry

    def wave1(q, carry):
        for w in range(2):
            first_in(q, w).wait_recv()
            second(q, w).start()
        for w in range(2):
            third(q, 1, w).start()
            third(q, 3, w).start()
        for w in range(2):
            third_in(q, 0, w).wait_recv()
            fourth(q, 0, w).start()
        return carry

    def wave2(q, carry):
        for w in range(2):
            second_in(q, w).wait_recv()
        for w in range(2):
            third(q, 2, w).start()
        for o in (1, 3):
            for w in range(2):
                third_in(q, o, w).wait_recv()
                fourth(q, o, w).start()
        return carry

    def wave3(q, carry):
        for w in range(2):
            third_in(q, 2, w).wait_recv()
            fourth(q, 2, w).start()
        return carry

    def wave4(q, carry):
        for o in range(4):
            for w in range(2):
                fourth_in(q, o, w).wait_recv()
        across(q, e).start()
        return carry

    def wave5(q, carry):
        across(q, 1 - e).wait_recv()
        return carry

    def level_copy(d):
        return remote(ostage.at[0], ostage.at[d], sp.at[d], rp.at[d], level(d))

    def core_copy():
        return remote(ostage.at[ny], ostage.at[ny + 1], sq, rq, twin)

    lax.fori_loop(0, CHUNKS, wave0, 0)
    for d in range(1, 16):
        off_copy(d).start()
    lax.fori_loop(0, CHUNKS, wave1, 0)
    top = offs[0]
    for d in range(1, 16):
        off_copy(d).wait_recv()
        top = jnp.maximum(top, offs[d])
    ostage[0] = top
    lax.fori_loop(0, CHUNKS, wave2, 0)
    for d in range(1, ny):
        level_copy(d).start()
    lax.fori_loop(0, CHUNKS, wave3, 0)
    for d in range(1, ny):
        level_copy(d).wait_recv()
        top = jnp.maximum(top, ostage[d])
    ostage[ny] = top
    lax.fori_loop(0, CHUNKS - 1, wave4, 0)
    core_copy().start()
    wave4(CHUNKS - 1, 0)
    lax.fori_loop(0, CHUNKS, wave5, 0)
    core_copy().wait_recv()
    omax_ref[...] = jnp.maximum(top, ostage[ny + 1])

    own_copy().wait_send()

    for d in range(1, 16):
        spread_copy(d).wait_send()
        pass_copy(d).wait_send()
        off_copy(d).wait_send()
    for d in range(1, ny):
        level_copy(d).wait_send()
    core_copy().wait_send()

    def drain_chunk(q, carry):
        for w in range(2):
            first(q, w).wait_send()
            second(q, w).wait_send()
            for o in range(4):
                third(q, o, w).wait_send()
                fourth(q, o, w).wait_send()
        across(q, e).wait_send()
        return carry

    lax.fori_loop(0, CHUNKS, drain_chunk, 0)


def gather(idx, blocks, packed, offs, ny):
    slots, length, width = packed.shape
    rows = length // 16
    vm = pl.BlockSpec(memory_space=pltpu.VMEM)
    dma = pltpu.SemaphoreType.DMA
    n = CHUNKS
    return pl.pallas_call(
        functools.partial(gather_kernel, ny),
        out_shape=(
            jax.ShapeDtypeStruct((16, blocks, rows, width), bf16),
            jax.ShapeDtypeStruct(offs.shape, f32),
        ),
        in_specs=[pl.BlockSpec(memory_space=pltpu.SMEM), vm, vm],
        out_specs=(vm, vm),
        scratch_shapes=[
            pltpu.VMEM((2, 16, slots, rows, width), bf16),
            pltpu.VMEM((16,) + offs.shape, f32),
            pltpu.VMEM((ny + 2,) + offs.shape, f32),
            dma((16,)), dma((16,)), dma((16,)), dma((16,)),
            dma((n, 2)), dma((n, 2)), dma((n, 2)), dma((n, 2)),
            dma((n, 4, 2)), dma((n, 4, 2)), dma((n, 4, 2)), dma((n, 4, 2)),
            dma((n,)), dma((n,)),
            dma((16,)), dma((16,)), dma((ny,)), dma((ny,)), dma, dma,
        ],
        compiler_params=pltpu.CompilerParams(
            collective_id=0, has_side_effects=True, vmem_limit_bytes=16 << 20
        ),
        cost_estimate=pl.CostEstimate(flops=20 * 10**9, bytes_accessed=1 << 20, transcendentals=0),
        name="gather_factors",
    )(idx, packed, offs)


def apply_kernel(p_ref, o_ref, g_ref, u_any, tops_ref, u_ref, f_ref, out_sem):
    blocks = g_ref.shape[0]
    rows = p_ref.shape[2]

    def save(k):
        return pltpu.make_async_copy(u_ref.at[k], u_any.at[k], out_sem.at[k])

    for i in range(MAXS):
        tops_ref[i] = jnp.max(o_ref[i : i + 1, :])

    def assemble(k, slot):
        packed = p_ref[:, k].reshape(p_ref.shape[0] * rows, GW)
        for t, (i, j) in enumerate(TILES):
            tile = packed[grp(t)]
            f_ref[slot, grp(i), grp(j)] = tile
            if i != j:
                f_ref[slot, grp(j), grp(i)] = tile.T

    def turn(k, slot):
        u_ref[k] = dot(g_ref[k], f_ref[slot]).astype(bf16)

    assemble(0, 0)

    def step(n, carry):
        k = 2 * n
        assemble(k + 1, 1)
        turn(k, 0)
        assemble(jnp.minimum(k + 2, blocks - 1), 0)
        turn(k + 1, 1)
        save(k).start()
        save(k + 1).start()
        return carry

    lax.fori_loop(0, blocks // 2, step, 0)
    for k in range(blocks):
        save(k).wait()


def apply(packed, tops, gradients):
    blocks, cols, size = gradients.shape
    anywhere = pl.BlockSpec(memory_space=pl.ANY)
    vm = pl.BlockSpec(memory_space=pltpu.VMEM)
    return pl.pallas_call(
        apply_kernel,
        out_shape=(
            jax.ShapeDtypeStruct((blocks, cols, size), bf16),
            jax.ShapeDtypeStruct((MAXS,), f32),
        ),
        in_specs=[vm, vm, vm],
        out_specs=(anywhere, pl.BlockSpec(memory_space=pltpu.SMEM)),
        scratch_shapes=[
            pltpu.VMEM((blocks, cols, size), bf16),
            pltpu.VMEM((2, size, size), bf16),
            pltpu.SemaphoreType.DMA((blocks,)),
        ],
        compiler_params=pltpu.CompilerParams(vmem_limit_bytes=28 << 20),
        name="apply_factors",
    )(packed, tops, gradients)


BLK = AXES[:3]


def per_device(ny, statistics, gradients, live_counts, slot_row, sweeps):
    matrices = statistics[0]
    live_counts, slot_row, sweeps, matrices = (
        pltpu.with_memory_space_constraint(value, pltpu.HBM)
        for value in (live_counts, slot_row, sweeps, matrices)
    )
    packed, offs, where_of = jacobi(
        live_counts, slot_row, sweeps, gradients.shape[1], matrices
    )
    pieces, tops = gather(where_of, gradients.shape[1], packed, offs, ny)
    updates, off_max = apply(pieces, tops, jnp.swapaxes(gradients[0], 1, 2))
    return jnp.swapaxes(updates, 1, 2)[None], off_max


def solution(mesh):
    ny = mesh.shape["grp"]
    split_mesh = Mesh(mesh.devices.reshape(4, 4, 2, ny), AXES)
    return jax.shard_map(
        functools.partial(per_device, ny),
        mesh=split_mesh,
        in_specs=(
            P("grp", BLK, None, None),
            P("grp", None, None, BLK),
            P("grp", None),
            P("grp", None),
            P("grp", BLK),
        ),
        out_specs=(P("grp", None, None, BLK), P()),
        check_vma=False,
    )
```
